16 devices in a mesh: data: 2 (over y, z), tp: 8 (over x, core).
Axes of the slice: x: 4, y: 2, z: 1, core: 2. Of those that a mesh axis runs over, the one named last changes fastest.
The devices are a block of a 4x4x8 slice.
Arguments:
- x_in: bfloat16 [16384, 2048], P('data'), parts along dimension 0
- w_gate: bfloat16 [2048, 8192], P(None, 'tp')
- w_up: bfloat16 [2048, 8192], P(None, 'tp')
- w_down: bfloat16 [8192, 2048], P('tp')
- residual: bfloat16 [16384, 2048], P(('data', 'tp')), parts along dimension 0
- norm_gain: float32 [2048], replicated
Outputs:
- output 1: bfloat16 [16384, 2048], P(('data', 'tp')), parts along dimension 0
- output 2: bfloat16 [16384, 2048], P(('data', 'tp')), parts along dimension 0
There are 2 independent parts. The reference program is written for one: setup_inputs(seed, part) draws one part's arguments, and reference() takes and returns one part's arrays. A program takes and returns all parts, laid end to end along the dimension named above; an argument that names none is the same for every part.
All inputs are finite; a program needn't handle non-finite values.
Results may differ from the reference program's by a relative error of at most 0.00647883.
Values are sent between devices in bfloat16 or wider.
A program may use at most 768 MiB of HBM per device.

```python
import jax
import jax.numpy as jnp
from jax import lax

T = 8192
D = 2048
F = 8192
TP = 8
F_SHARD = F // TP
EPS = 1e-5


def setup_inputs(seed: int = 0, part: int = 0) -> dict:
    key = jax.random.key(seed)
    shared = jax.random.split(key, 4)
    local = jax.random.split(jax.random.fold_in(key, part), 2)
    x_in = jax.random.normal(local[0], (T, D), jnp.float32).astype(jnp.bfloat16)
    residual = jax.random.normal(local[1], (T, D), jnp.float32).astype(jnp.bfloat16)
    w_gate = (jax.random.normal(shared[0], (D, F), jnp.float32) * D ** -0.5).astype(jnp.bfloat16)
    w_up = (jax.random.normal(shared[1], (D, F), jnp.float32) * D ** -0.5).astype(jnp.bfloat16)
    w_down = (jax.random.normal(shared[2], (F, D), jnp.float32) * (2.0 / F) ** 0.5).astype(jnp.bfloat16)
    norm_gain = 1.0 + 0.3 * jax.random.normal(shared[3], (D,), jnp.float32)
    return {"x_in": x_in, "w_gate": w_gate, "w_up": w_up, "w_down": w_down, "residual": residual, "norm_gain": norm_gain}


def reference(x_in, w_gate, w_up, w_down, residual, norm_gain):
    gate_shards = w_gate.reshape(D, TP, F_SHARD).transpose(1, 0, 2)
    up_shards = w_up.reshape(D, TP, F_SHARD).transpose(1, 0, 2)
    down_shards = w_down.reshape(TP, F_SHARD, D)

    def add_shard(running, shard_w):
        gate_cols, up_cols, down_rows = shard_w
        gate_val = jnp.dot(x_in, gate_cols, preferred_element_type=jnp.float32)
        up_val = jnp.dot(x_in, up_cols, preferred_element_type=jnp.float32)
        hidden = (jax.nn.silu(gate_val) * up_val).astype(jnp.bfloat16)
        part_prod = jnp.dot(hidden, down_rows, preferred_element_type=jnp.float32).astype(jnp.bfloat16)
        return running + part_prod.astype(jnp.float32), None

    y_sum = lax.scan(add_shard, jnp.zeros((T, D), jnp.float32), (gate_shards, up_shards, down_shards))[0]
    hidden_sum = residual.astype(jnp.float32) + y_sum
    mean_sq = jnp.mean(hidden_sum * hidden_sum, axis=-1, keepdims=True)
    normed = hidden_sum * lax.rsqrt(mean_sq + EPS) * norm_gain
    return hidden_sum.astype(jnp.bfloat16), normed.astype(jnp.bfloat16)
```

```python
import functools

import jax
import jax.numpy as jnp
from jax import lax
from jax.experimental import pallas as pl
from jax.experimental.pallas import tpu as pltpu
from jax.sharding import PartitionSpec as P

EPS = 1e-5
CORES = 2
ROWS = 128
SLOTS = 3
RIGHT, LEFT = 0, 1


def ring_kernel(
    n, x_in, w_gate, w_up, w_down, residual, h_out, mid_in, near_in,
    gate_w, up_w, down_w, x_tile, hidden, mid_out, stage, far_in, acc, extra, mid_tile, res_tile,
    w_sem, peer_send, peer_recv, x_sem, mid_send, mid_recv, stage_send, near_recv, far_recv, extra_sem, mid_sem, res_sem, out_sem,
):
    me = lax.axis_index("tp")
    chips = n // CORES
    chip, core = me // CORES, lax.rem(me, CORES)
    own_rows = residual.shape[0]
    half = own_rows // 2
    tiles = half // ROWS
    depth, width = w_gate.shape[1], w_down.shape[1]

    def device(c, k):
        return {"tp": lax.rem(c + chips, chips) * CORES + k}

    right, left, peer = device(chip + 1, core), device(chip - 1, core), device(chip, 1 - core)
    next_dev = (right, left)

    def x_copies(stg, t, slot):
        (c0, h0), (c1, h1) = (
            ((chip + 2, 0), (chip + 2, 1)),
            ((chip + 2, 0), (chip + 2, 1)),
            ((chip + 1, 1), (chip - 1, 0)),
            ((chip + 1, 0), (chip - 1, 1)),
            ((chip, 0), (chip, 1)),
        )[stg]
        out = []
        for d, (c, h) in enumerate(((c0, h0), (c1, h1))):
            c = lax.rem(c + chips, chips)
            row = pl.multiple_of((c * CORES + core) * own_rows + h * half + t * ROWS, ROWS)
            out.append(pltpu.make_async_copy(
                x_in.at[pl.ds(row, ROWS)], x_tile.at[slot, pl.ds(d * ROWS, ROWS)], x_sem.at[slot, d]))
        return out

    def start_x(stg, t, slot):
        for cp in x_copies(stg, t, slot):
            cp.start()

    def wait_x(stg, t, slot):
        for cp in x_copies(stg, t, slot):
            cp.wait()

    own_w = [
        pltpu.make_async_copy(w_gate, gate_w.at[0], w_sem.at[0]),
        pltpu.make_async_copy(w_up, up_w.at[0], w_sem.at[1]),
        pltpu.make_async_copy(w_down, down_w.at[0], w_sem.at[2]),
    ]
    start_x(0, 0, 0)
    for cp in own_w:
        cp.start()

    barrier = pltpu.get_barrier_semaphore()
    for dev in (peer, left, right):
        pl.semaphore_signal(barrier, inc=1, device_id=dev, device_id_type=pl.DeviceIdType.MESH)
    pl.semaphore_wait(barrier, 3)

    def remote(src, dst, send, recv, dev):
        return pltpu.make_async_remote_copy(
            src_ref=src, dst_ref=dst, send_sem=send, recv_sem=recv, device_id=dev, device_id_type=pl.DeviceIdType.MESH)

    peer_w = [
        remote(w_gate, gate_w.at[1], peer_send.at[0], peer_recv.at[0], peer),
        remote(w_up, up_w.at[1], peer_send.at[1], peer_recv.at[1], peer),
        remote(w_down, down_w.at[1], peer_send.at[2], peer_recv.at[2], peer),
    ]
    for cp in peer_w:
        cp.start()

    def rows_of(t):
        return pl.ds(pl.multiple_of(t * ROWS, ROWS), ROWS)

    def mid_copy(d, s, t):
        return remote(mid_out.at[s, d, rows_of(t)], mid_in.at[d, s, rows_of(t)],
                      mid_send.at[s, d, t], mid_recv.at[s, d, t], next_dev[d])

    def near_copy(d, t, slot):
        return remote(stage.at[slot, d], near_in.at[d, rows_of(t)], stage_send.at[slot, d], near_recv.at[d, t], next_dev[d])

    def far_copy(d, t, slot):
        return remote(stage.at[slot, d], far_in.at[d, rows_of(t)], stage_send.at[slot, d], far_recv.at[d, t], next_dev[d])

    def make_hidden(slot, s):
        def chunk(j, _):
            cols = pl.ds(pl.multiple_of(j * 256, 256), 256)
            x = x_tile[slot]
            gate = jnp.dot(x, gate_w[s, :, cols], preferred_element_type=jnp.float32)
            up = jnp.dot(x, up_w[s, :, cols], preferred_element_type=jnp.float32)
            hidden[s, :, cols] = (jax.nn.silu(gate) * up).astype(jnp.bfloat16)
            return 0
        lax.fori_loop(0, depth // 256, chunk, 0)

    def part(s, cols):
        return jnp.dot(hidden[s], down_w[s, :, cols], preferred_element_type=jnp.float32).astype(jnp.bfloat16)

    def both(slot, store):
        make_hidden(slot, 0)
        make_hidden(slot, 1)

        def chunk(j, _):
            cols = pl.ds(pl.multiple_of(j * 512, 512), 512)
            store(cols, part(0, cols).astype(jnp.float32) + part(1, cols).astype(jnp.float32))
            return 0
        lax.fori_loop(0, width // 512, chunk, 0)

    def next_x(stg, t, slot):
        @pl.when(t < tiles - 1)
        def _():
            start_x(stg, t + 1, 1 - slot)
        if stg < 4:
            @pl.when(t == tiles - 1)
            def _():
                start_x(stg + 1, 0, 1 - slot)

    for s in range(2):
        for w in range(3) if s == 0 else ():
            own_w[w].wait()
        if s == 1:
            for cp in peer_w:
                cp.wait_recv()

        def mid_step(t, _, s=s):
            slot = lax.rem(t, 2)
            next_x(s, t, slot)
            wait_x(s, t, slot)
            make_hidden(slot, s)

            def chunk(j, _):
                cols = pl.ds(pl.multiple_of(j * 512, 512), 512)
                y = part(s, cols)
                mid_out[s, RIGHT, rows_of(t), cols] = y[:ROWS]
                mid_out[s, LEFT, rows_of(t), cols] = y[ROWS:]
                return 0
            lax.fori_loop(0, width // 512, chunk, 0)
            for d in (RIGHT, LEFT):
                mid_copy(d, s, t).start()
            return 0
        lax.fori_loop(0, tiles, mid_step, 0)

    def near_step(t, _):
        slot, place = lax.rem(t, 2), lax.rem(t, SLOTS)
        next_x(2, t, slot)
        wait_x(2, t, slot)

        @pl.when(t >= SLOTS)
        def _():
            for d in (RIGHT, LEFT):
                near_copy(d, t - SLOTS, place).wait_send()

        def store(cols, y):
            stage[place, RIGHT, :, cols] = y[:ROWS]
            stage[place, LEFT, :, cols] = y[ROWS:]
        both(slot, store)
        for d in (RIGHT, LEFT):
            near_copy(d, t, place).start()
        return 0
    lax.fori_loop(0, tiles, near_step, 0)

    def mid_loads(t):
        return [pltpu.make_async_copy(mid_in.at[d, s, rows_of(t)], mid_tile.at[d, s], mid_sem.at[d, s])
                for d in (RIGHT, LEFT) for s in (0, 1)]

    def far_step(t, _):
        slot, place = lax.rem(t, 2), lax.rem(t + tiles, SLOTS)
        next_x(3, t, slot)
        wait_x(3, t, slot)
        for d in (RIGHT, LEFT):
            near_copy(d, t, place).wait_send()

        def store(cols, y):
            stage[place, RIGHT, :, cols] = y[:ROWS]
            stage[place, LEFT, :, cols] = y[ROWS:]
        both(slot, store)
        for d in (RIGHT, LEFT):
            for s in (0, 1):
                mid_copy(d, s, t).wait_recv()
        for cp in mid_loads(t):
            cp.start()
        for cp in mid_loads(t):
            cp.wait()

        def add(j, _):
            r = pl.ds(pl.multiple_of(j * 16, 16), 16)
            for d in (RIGHT, LEFT):
                stage[place, d, r] += mid_tile[d, 0, r].astype(jnp.float32) + mid_tile[d, 1, r].astype(jnp.float32)
            return 0
        lax.fori_loop(0, ROWS // 16, add, 0)
        for d in (RIGHT, LEFT):
            far_copy(d, t, place).start()
        return 0
    lax.fori_loop(0, tiles, far_step, 0)

    def own_loads(t):
        out = []
        for h in (0, 1):
            row = pl.multiple_of(h * half + t * ROWS, ROWS)
            out.append(pltpu.make_async_copy(near_in.at[1 - h, rows_of(t)], extra.at[h], extra_sem.at[h]))
            out.append(pltpu.make_async_copy(residual.at[pl.ds(row, ROWS)], res_tile.at[h], res_sem.at[h]))
        return out

    def own_step(t, _):
        slot = lax.rem(t, 2)
        next_x(4, t, slot)
        wait_x(4, t, slot)

        def store(cols, y):
            acc[0, rows_of(t), cols] = y[:ROWS]
            acc[1, rows_of(t), cols] = y[ROWS:]
        both(slot, store)
        for d in (RIGHT, LEFT):
            near_copy(d, t, 0).wait_recv()
        for cp in own_loads(t):
            cp.start()
        for cp in own_loads(t):
            cp.wait()

        def add(j, _):
            r = pl.ds(pl.multiple_of(j * 16, 16), 16)
            here = pl.ds(pl.multiple_of(t * ROWS + j * 16, 16), 16)
            for h in (0, 1):
                acc[h, here] += extra[h, r] + res_tile[h, r].astype(jnp.float32)
            return 0
        lax.fori_loop(0, ROWS // 16, add, 0)
        return 0
    lax.fori_loop(0, tiles, own_step, 0)

    def out_copies(t):
        return [pltpu.make_async_copy(
            acc.at[h, rows_of(t)], h_out.at[pl.ds(pl.multiple_of(h * half + t * ROWS, ROWS), ROWS)], out_sem.at[h, t])
            for h in (0, 1)]

    def last_step(t, _):
        for d in (RIGHT, LEFT):
            far_copy(d, t, 0).wait_recv()

        def add(j, _):
            here = pl.ds(pl.multiple_of(t * ROWS + j * 16, 16), 16)
            for h in (0, 1):
                acc[h, here] += far_in[h, here]
            return 0
        lax.fori_loop(0, ROWS // 16, add, 0)
        for cp in out_copies(t):
            cp.start()
        return 0
    lax.fori_loop(0, tiles, last_step, 0)

    for cp in peer_w:
        cp.wait_send()

    def drain(t, _):
        for d in (RIGHT, LEFT):
            for s in (0, 1):
                mid_copy(d, s, t).wait_send()
        for cp in out_copies(t):
            cp.wait()
        return 0
    lax.fori_loop(0, tiles, drain, 0)

    def drain_stage(i, _):
        for d in (RIGHT, LEFT):
            far_copy(d, 0, i).wait_send()
        return 0
    lax.fori_loop(0, SLOTS, drain_stage, 0)


def norm_kernel(h, gain, h_out, normed):
    value = h[...]
    mean_sq = jnp.mean(value * value, axis=-1, keepdims=True)
    h_out[...] = value.astype(jnp.bfloat16)
    normed[...] = (value * lax.rsqrt(mean_sq + EPS) * gain[...]).astype(jnp.bfloat16)


def solution(mesh):
    n = mesh.shape["tp"]

    def local_block(x_in, w_gate, w_up, w_down, residual, norm_gain):
        rows, width = residual.shape
        depth = w_gate.shape[1]
        half = rows // 2
        tiles = half // ROWS
        f32, bf16 = jnp.float32, jnp.bfloat16
        dma = pltpu.SemaphoreType.DMA
        h, _, _ = pl.pallas_call(
            functools.partial(ring_kernel, n),
            out_shape=(
                jax.ShapeDtypeStruct((rows, width), f32),
                jax.ShapeDtypeStruct((2, 2, half, width), bf16),
                jax.ShapeDtypeStruct((2, half, width), f32),
            ),
            in_specs=[pl.BlockSpec(memory_space=pl.ANY)] * 5,
            out_specs=(pl.BlockSpec(memory_space=pl.ANY),) * 3,
            scratch_shapes=[
                pltpu.VMEM((2,) + w_gate.shape, bf16),
                pltpu.VMEM((2,) + w_up.shape, bf16),
                pltpu.VMEM((2,) + w_down.shape, bf16),
                pltpu.VMEM((2, 2 * ROWS, width), bf16),
                pltpu.VMEM((2, 2 * ROWS, depth), bf16),
                pltpu.VMEM((2, 2, half, width), bf16),
                pltpu.VMEM((SLOTS, 2, ROWS, width), f32),
                pltpu.VMEM((2, half, width), f32),
                pltpu.VMEM((2, half, width), f32),
                pltpu.VMEM((2, ROWS, width), f32),
                pltpu.VMEM((2, 2, ROWS, width), bf16),
                pltpu.VMEM((2, ROWS, width), bf16),
                dma((3,)), dma((3,)), dma((3,)),
                dma((2, 2)),
                dma((2, 2, tiles)), dma((2, 2, tiles)),
                dma((SLOTS, 2)), dma((2, tiles)), dma((2, tiles)),
                dma((2,)), dma((2, 2)), dma((2,)), dma((2, tiles)),
            ],
            compiler_params=pltpu.CompilerParams(
                collective_id=0, has_side_effects=True, vmem_limit_bytes=66_000_000),
            name="ring",
        )(x_in, w_gate, w_up, w_down, residual)
        row_block = pl.BlockSpec((ROWS, width), lambda i: (i, 0))
        return pl.pallas_call(
            norm_kernel,
            grid=(rows // ROWS,),
            out_shape=(jax.ShapeDtypeStruct((rows, width), bf16),) * 2,
            in_specs=[row_block, pl.BlockSpec((1, width), lambda i: (0, 0))],
            out_specs=(row_block, row_block),
            name="norm",
        )(h, norm_gain.reshape(1, width))

    row_spec = P(("data", "tp"), None)
    return jax.shard_map(local_block, mesh=mesh, in_specs=(P("data", None), P(None, "tp"), P(None, "tp"), P("tp", None), row_spec, P(None)), out_specs=(row_spec, row_spec), check_vma=False)
```

```python
import functools

import jax
import jax.numpy as jnp
from jax import lax
from jax.experimental import pallas as pl
from jax.experimental.pallas import tpu as pltpu
from jax.sharding import PartitionSpec as P

EPS = 1e-5
CORES = 2
ROWS = 128
SLOTS = 3
SUB = 32
WCOLS = 256
RIGHT, LEFT = 0, 1


def ring_kernel(
    n, x_in, w_gate, w_up, w_down, residual, norm_gain, result, mid_in, near_in,
    gate_w, up_w, down_w, x_tile, hidden, stage, far_in, acc, extra, mid_tile, res_tile, gain,
    gate_sem, up_sem, down_sem, peer_send, peer_recv, x_sem, mid_send, mid_recv, stage_send, near_recv, far_recv, last_send,
    last_recv, extra_sem, mid_sem, res_sem, gain_sem,
):
    me = lax.axis_index("tp")
    chips = n // CORES
    chip, core = me // CORES, lax.rem(me, CORES)
    own_rows = residual.shape[0]
    half = own_rows // 2
    tiles = half // ROWS
    depth, width = w_gate.shape[1], w_down.shape[1]

    def device(c, k):
        return {"tp": lax.rem(c + chips, chips) * CORES + k}

    right, left, peer = device(chip + 1, core), device(chip - 1, core), device(chip, 1 - core)
    next_dev = (right, left)
    last_place = (2 * tiles - 1) % SLOTS

    def x_copies(stg, t, slot):
        (c0, h0), (c1, h1) = (
            ((chip + 2, 0), (chip + 2, 1)),
            ((chip + 2, 0), (chip + 2, 1)),
            ((chip + 1, 1), (chip - 1, 0)),
            ((chip + 1, 0), (chip - 1, 1)),
            ((chip, 0), (chip, 1)),
        )[stg]
        out = []
        for d, (c, h) in enumerate(((c0, h0), (c1, h1))):
            c = lax.rem(c + chips, chips)
            row = pl.multiple_of((c * CORES + core) * own_rows + h * half + t * ROWS, ROWS)
            out.append(pltpu.make_async_copy(
                x_in.at[pl.ds(row, ROWS)], x_tile.at[slot, pl.ds(d * ROWS, ROWS)], x_sem.at[slot, d]))
        return out

    def start_x(stg, t, slot):
        for cp in x_copies(stg, t, slot):
            cp.start()

    def wait_x(stg, t, slot):
        for cp in x_copies(stg, t, slot):
            cp.wait()

    def own_cols(j):
        cols = pl.ds(pl.multiple_of(j * WCOLS, WCOLS), WCOLS)
        return [
            pltpu.make_async_copy(w_gate.at[:, cols], gate_w.at[0, :, cols], gate_sem.at[j]),
            pltpu.make_async_copy(w_up.at[:, cols], up_w.at[0, :, cols], up_sem.at[j]),
        ]

    own_down = pltpu.make_async_copy(w_down, down_w.at[0], down_sem)
    own_gain = pltpu.make_async_copy(norm_gain, gain, gain_sem)
    start_x(0, 0, 0)
    for j in range(depth // WCOLS):
        for cp in own_cols(j):
            cp.start()
    own_down.start()
    own_gain.start()

    barrier = pltpu.get_barrier_semaphore()
    for dev in (peer, left, right):
        pl.semaphore_signal(barrier, inc=1, device_id=dev, device_id_type=pl.DeviceIdType.MESH)
    pl.semaphore_wait(barrier, 3)

    def remote(src, dst, send, recv, dev):
        return pltpu.make_async_remote_copy(
            src_ref=src, dst_ref=dst, send_sem=send, recv_sem=recv, device_id=dev, device_id_type=pl.DeviceIdType.MESH)

    peer_w = [
        remote(w_gate, gate_w.at[1], peer_send.at[0], peer_recv.at[0], peer),
        remote(w_up, up_w.at[1], peer_send.at[1], peer_recv.at[1], peer),
        remote(w_down, down_w.at[1], peer_send.at[2], peer_recv.at[2], peer),
    ]
    for cp in peer_w:
        cp.start()

    def rows_of(t):
        return pl.ds(pl.multiple_of(t * ROWS, ROWS), ROWS)

    def mid_copy(d, s, t):
        return remote(result.at[s, d, rows_of(t)], mid_in.at[d, s, rows_of(t)],
                      mid_send.at[s, d, t], mid_recv.at[s, d, t], next_dev[d])

    def near_copy(d, t, slot):
        return remote(stage.at[slot, d], near_in.at[d, rows_of(t)], stage_send.at[slot, d], near_recv.at[d, t], next_dev[d])

    def far_copy(d, t, slot):
        return remote(stage.at[slot, d], far_in.at[d, rows_of(t)], stage_send.at[slot, d], far_recv.at[d, t], next_dev[d])

    def last_copy(d, i):
        here = pl.ds((tiles - 1) * ROWS + i * SUB, SUB)
        return remote(stage.at[last_place, d, pl.ds(i * SUB, SUB)], far_in.at[d, here],
                      last_send.at[d, i], last_recv.at[d, i], next_dev[d])

    def make_hidden(slot, s, first=False):
        def chunk(j, _):
            if first:
                for cp in own_cols(j):
                    cp.wait()
            cols = pl.ds(pl.multiple_of(j * WCOLS, WCOLS), WCOLS)
            x = x_tile[slot]
            gate = jnp.dot(x, gate_w[s, :, cols], preferred_element_type=jnp.float32)
            up = jnp.dot(x, up_w[s, :, cols], preferred_element_type=jnp.float32)
            hidden[s, :, cols] = (jax.nn.silu(gate) * up).astype(jnp.bfloat16)
            return 0
        lax.fori_loop(0, depth // WCOLS, chunk, 0)

    def part(s, cols):
        return jnp.dot(hidden[s], down_w[s, :, cols], preferred_element_type=jnp.float32).astype(jnp.bfloat16)

    def both(slot, store):
        make_hidden(slot, 0)
        make_hidden(slot, 1)

        def chunk(j, _):
            cols = pl.ds(pl.multiple_of(j * 512, 512), 512)
            store(cols, part(0, cols).astype(jnp.float32) + part(1, cols).astype(jnp.float32))
            return 0
        lax.fori_loop(0, width // 512, chunk, 0)

    def next_x(stg, t, slot):
        @pl.when(t < tiles - 1)
        def _():
            start_x(stg, t + 1, 1 - slot)
        if stg < 4:
            @pl.when(t == tiles - 1)
            def _():
                start_x(stg + 1, 0, 1 - slot)

    def mid_step(t, s, first=False):
            slot = lax.rem(t, 2)
            next_x(s, t, slot)
            wait_x(s, t, slot)
            make_hidden(slot, s, first)
            if first:
                own_down.wait()

            def chunk(j, _):
                cols = pl.ds(pl.multiple_of(j * 512, 512), 512)
                y = part(s, cols)
                result[s, RIGHT, rows_of(t), cols] = y[:ROWS]
                result[s, LEFT, rows_of(t), cols] = y[ROWS:]
                return 0
            lax.fori_loop(0, width // 512, chunk, 0)
            for d in (RIGHT, LEFT):
                mid_copy(d, s, t).start()

    mid_step(jnp.int32(0), 0, first=True)

    def mid_loop(s, t0):
        def step(t, _):
            mid_step(t, s)
            return 0
        lax.fori_loop(t0, tiles, step, 0)

    mid_loop(0, 1)
    for cp in peer_w:
        cp.wait_recv()
    mid_loop(1, 0)

    def near_step(t, _):
        slot, place = lax.rem(t, 2), lax.rem(t, SLOTS)
        next_x(2, t, slot)
        wait_x(2, t, slot)

        @pl.when(t >= SLOTS)
        def _():
            for d in (RIGHT, LEFT):
                near_copy(d, t - SLOTS, place).wait_send()

        def store(cols, y):
            stage[place, RIGHT, :, cols] = y[:ROWS]
            stage[place, LEFT, :, cols] = y[ROWS:]
        both(slot, store)
        for d in (RIGHT, LEFT):
            near_copy(d, t, place).start()
        return 0
    lax.fori_loop(0, tiles, near_step, 0)

    def mid_loads(t):
        return [pltpu.make_async_copy(mid_in.at[d, s, rows_of(t)], mid_tile.at[d, s], mid_sem.at[d, s])
                for d in (RIGHT, LEFT) for s in (0, 1)]

    def far_step(t, _):
        slot, place = lax.rem(t, 2), lax.rem(t + tiles, SLOTS)
        next_x(3, t, slot)
        wait_x(3, t, slot)
        for d in (RIGHT, LEFT):
            near_copy(d, t, place).wait_send()

        def store(cols, y):
            stage[place, RIGHT, :, cols] = y[:ROWS]
            stage[place, LEFT, :, cols] = y[ROWS:]
        both(slot, store)
        for d in (RIGHT, LEFT):
            for s in (0, 1):
                mid_copy(d, s, t).wait_recv()
        for cp in mid_loads(t):
            cp.start()
        for cp in mid_loads(t):
            cp.wait()

        def add(j, _):
            r = pl.ds(pl.multiple_of(j * 16, 16), 16)
            for d in (RIGHT, LEFT):
                stage[place, d, r] += mid_tile[d, 0, r].astype(jnp.float32) + mid_tile[d, 1, r].astype(jnp.float32)
            return 0
        lax.fori_loop(0, ROWS // 16, add, 0)

        @pl.when(t < tiles - 1)
        def _():
            for d in (RIGHT, LEFT):
                far_copy(d, t, place).start()

        @pl.when(t == tiles - 1)
        def _():
            for i in range(ROWS // SUB):
                for d in (RIGHT, LEFT):
                    last_copy(d, i).start()
        return 0
    lax.fori_loop(0, tiles, far_step, 0)

    def own_loads(t):
        out = []
        for h in (0, 1):
            row = pl.multiple_of(h * half + t * ROWS, ROWS)
            out.append(pltpu.make_async_copy(near_in.at[1 - h, rows_of(t)], extra.at[h], extra_sem.at[h]))
            out.append(pltpu.make_async_copy(residual.at[pl.ds(row, ROWS)], res_tile.at[h], res_sem.at[h]))
        return out

    def own_step(t, _):
        slot = lax.rem(t, 2)
        next_x(4, t, slot)
        wait_x(4, t, slot)

        def store(cols, y):
            acc[0, rows_of(t), cols] = y[:ROWS]
            acc[1, rows_of(t), cols] = y[ROWS:]
        both(slot, store)
        for d in (RIGHT, LEFT):
            near_copy(d, t, 0).wait_recv()
        for cp in own_loads(t):
            cp.start()
        for cp in own_loads(t):
            cp.wait()

        def add(j, _):
            r = pl.ds(pl.multiple_of(j * 16, 16), 16)
            here = pl.ds(pl.multiple_of(t * ROWS + j * 16, 16), 16)
            for h in (0, 1):
                acc[h, here] += extra[h, r] + res_tile[h, r].astype(jnp.float32)
            return 0
        lax.fori_loop(0, ROWS // 16, add, 0)
        return 0
    lax.fori_loop(0, tiles, own_step, 0)

    for cp in peer_w:
        cp.wait_send()

    def drain(t, _):
        for d in (RIGHT, LEFT):
            for s in (0, 1):
                mid_copy(d, s, t).wait_send()
        return 0
    lax.fori_loop(0, tiles, drain, 0)
    own_gain.wait()

    def finish(row):
        for h in (0, 1):
            here = pl.ds(row, 16)
            value = acc[h, here] + far_in[h, here]
            mean_sq = jnp.mean(value * value, axis=-1, keepdims=True)
            result[0, h, here] = value.astype(jnp.bfloat16)
            result[1, h, here] = (value * lax.rsqrt(mean_sq + EPS) * gain[...]).astype(jnp.bfloat16)

    def last_step(t, _):
        for d in (RIGHT, LEFT):
            far_copy(d, t, 0).wait_recv()

        def rows16(j, _):
            finish(pl.multiple_of(t * ROWS + j * 16, 16))
            return 0
        lax.fori_loop(0, ROWS // 16, rows16, 0)
        return 0
    lax.fori_loop(0, tiles - 1, last_step, 0)

    for place in range(SLOTS):
        if place != last_place:
            for d in (RIGHT, LEFT):
                far_copy(d, 0, place).wait_send()

    for i in range(ROWS // SUB):
        for d in (RIGHT, LEFT):
            last_copy(d, i).wait_recv()
        for j in range(SUB // 16):
            finish((tiles - 1) * ROWS + i * SUB + j * 16)
    for i in range(ROWS // SUB):
        for d in (RIGHT, LEFT):
            last_copy(d, i).wait_send()


def write_kernel(result, h_out, normed, sem):
    half = result.shape[2]
    copies = [
        pltpu.make_async_copy(result.at[i, h], out.at[pl.ds(h * half, half)], sem.at[i, h])
        for i, out in enumerate((h_out, normed)) for h in (0, 1)]
    for cp in copies:
        cp.start()
    for cp in copies:
        cp.wait()


def solution(mesh):
    n = mesh.shape["tp"]

    def local_block(x_in, w_gate, w_up, w_down, residual, norm_gain):
        rows, width = residual.shape
        depth = w_gate.shape[1]
        half = rows // 2
        tiles = half // ROWS
        f32, bf16 = jnp.float32, jnp.bfloat16
        dma = pltpu.SemaphoreType.DMA
        any_space = pl.BlockSpec(memory_space=pl.ANY)
        result, _, _ = pl.pallas_call(
            functools.partial(ring_kernel, n),
            out_shape=(
                pltpu.VMEM((2, 2, half, width), bf16),
                jax.ShapeDtypeStruct((2, 2, half, width), bf16),
                jax.ShapeDtypeStruct((2, half, width), f32),
            ),
            in_specs=[any_space] * 6,
            out_specs=(pl.BlockSpec(memory_space=pltpu.VMEM), any_space, any_space),
            scratch_shapes=[
                pltpu.VMEM((2,) + w_gate.shape, bf16),
                pltpu.VMEM((2,) + w_up.shape, bf16),
                pltpu.VMEM((2,) + w_down.shape, bf16),
                pltpu.VMEM((2, 2 * ROWS, width), bf16),
                pltpu.VMEM((2, 2 * ROWS, depth), bf16),
                pltpu.VMEM((SLOTS, 2, ROWS, width), f32),
                pltpu.VMEM((2, half, width), f32),
                pltpu.VMEM((2, half, width), f32),
                pltpu.VMEM((2, ROWS, width), f32),
                pltpu.VMEM((2, 2, ROWS, width), bf16),
                pltpu.VMEM((2, ROWS, width), bf16),
                pltpu.VMEM((1, width), f32),
                dma((depth // WCOLS,)), dma((depth // WCOLS,)), dma(()), dma((3,)), dma((3,)),
                dma((2, 2)),
                dma((2, 2, tiles)), dma((2, 2, tiles)),
                dma((SLOTS, 2)), dma((2, tiles)), dma((2, tiles)),
                dma((2, ROWS // SUB)), dma((2, ROWS // SUB)),
                dma((2,)), dma((2, 2)), dma((2,)), dma(()),
            ],
            compiler_params=pltpu.CompilerParams(
                collective_id=0, has_side_effects=True, vmem_limit_bytes=55 * 2**20),
            name="ring",
        )(x_in, w_gate, w_up, w_down, residual, norm_gain.reshape(1, width))
        return pl.pallas_call(
            write_kernel,
            out_shape=(jax.ShapeDtypeStruct((rows, width), bf16),) * 2,
            in_specs=[pl.BlockSpec(memory_space=pltpu.VMEM)],
            out_specs=(any_space, any_space),
            scratch_shapes=[dma((2, 2))],
            compiler_params=pltpu.CompilerParams(vmem_limit_bytes=2**20),
            name="write",
        )(pltpu.with_memory_space_constraint(result, pltpu.VMEM))

    row_spec = P(("data", "tp"), None)
    return jax.shard_map(local_block, mesh=mesh, in_specs=(P("data", None), P(None, "tp"), P(None, "tp"), P("tp", None), row_spec, P(None)), out_specs=(row_spec, row_spec), check_vma=False)
```

```python
import functools

import jax
import jax.numpy as jnp
from jax import lax
from jax.experimental import pallas as pl
from jax.experimental.pallas import tpu as pltpu
from jax.sharding import PartitionSpec as P

EPS = 1e-5
CORES = 2
ROWS = 128
SLOTS = 3
SUB = 32
FIRST = 64
WCOLS = 256
YCOLS = 512
AHEAD = 4
RIGHT, LEFT = 0, 1


def ring_kernel(
    n, x_in, w_gate, w_up, w_down, residual, norm_gain, result, mid_in, near_in,
    gate_w, up_w, down_w, x_tile, hidden, stage, far_in, acc, extra, mid_tile, res_tile, gain,
    gate_sem, up_sem, down_sem, peer_send, peer_recv, x_sem, mid_send, mid_recv, stage_send, near_recv, far_recv, last_send,
    last_recv, extra_sem, mid_sem, res_sem, gain_sem, piece_sem, piece_send, piece_recv,
):
    me = lax.axis_index("tp")
    chips = n // CORES
    chip, core = me // CORES, lax.rem(me, CORES)
    own_rows = residual.shape[0]
    half = own_rows // 2
    tiles = half // ROWS
    depth, width = w_gate.shape[1], w_down.shape[1]

    def device(c, k):
        return {"tp": lax.rem(c + chips, chips) * CORES + k}

    right, left, peer = device(chip + 1, core), device(chip - 1, core), device(chip, 1 - core)
    next_dev = (right, left)
    last_place = (2 * tiles - 1) % SLOTS

    def x_copies(stg, t, slot):
        (c0, h0), (c1, h1) = (
            ((chip + 2, 0), (chip + 2, 1)),
            ((chip + 2, 0), (chip + 2, 1)),
            ((chip + 1, 1), (chip - 1, 0)),
            ((chip + 1, 0), (chip - 1, 1)),
            ((chip, 0), (chip, 1)),
        )[stg]
        out = []
        for d, (c, h) in enumerate(((c0, h0), (c1, h1))):
            c = lax.rem(c + chips, chips)
            row = pl.multiple_of((c * CORES + core) * own_rows + h * half + t * ROWS, ROWS)
            out.append(pltpu.make_async_copy(
                x_in.at[pl.ds(row, ROWS)], x_tile.at[slot, pl.ds(d * ROWS, ROWS)], x_sem.at[slot, d]))
        return out

    def start_x(stg, t, slot):
        for cp in x_copies(stg, t, slot):
            cp.start()

    def wait_x(stg, t, slot):
        for cp in x_copies(stg, t, slot):
            cp.wait()

    def piece_copies(i):
        out = []
        for d in (RIGHT, LEFT):
            row = pl.multiple_of((lax.rem(chip + 2, chips) * CORES + core) * own_rows + d * half + i * FIRST, FIRST)
            out.append(pltpu.make_async_copy(
                x_in.at[pl.ds(row, FIRST)], x_tile.at[0, pl.ds((2 * i + d) * FIRST, FIRST)], piece_sem.at[i, d]))
        return out

    def own_cols(j):
        cols = pl.ds(pl.multiple_of(j * WCOLS, WCOLS), WCOLS)
        return [
            pltpu.make_async_copy(w_gate.at[:, cols], gate_w.at[0, :, cols], gate_sem.at[j]),
            pltpu.make_async_copy(w_up.at[:, cols], up_w.at[0, :, cols], up_sem.at[j]),
        ]

    def own_down(j):
        cols = pl.ds(pl.multiple_of(j * YCOLS, YCOLS), YCOLS)
        return pltpu.make_async_copy(w_down.at[:, cols], down_w.at[0, :, cols], down_sem.at[j])

    own_gain = pltpu.make_async_copy(norm_gain, gain, gain_sem)
    loads = [own_cols(j) for j in range(depth // WCOLS)] + [[own_down(j)] for j in range(width // YCOLS)]

    def start_load(i):
        for cp in loads[i] if i < len(loads) else ():
            cp.start()

    def wait_load(i):
        for cp in loads[i]:
            cp.wait()
        start_load(i + AHEAD)

    for cp in piece_copies(0):
        cp.start()
    for i in range(AHEAD):
        start_load(i)
    for k in range(1, ROWS // FIRST):
        for cp in piece_copies(k):
            cp.start()

    barrier = pltpu.get_barrier_semaphore()
    for dev in (peer, left, right):
        pl.semaphore_signal(barrier, inc=1, device_id=dev, device_id_type=pl.DeviceIdType.MESH)

    def remote(src, dst, send, recv, dev):
        return pltpu.make_async_remote_copy(
            src_ref=src, dst_ref=dst, send_sem=send, recv_sem=recv, device_id=dev, device_id_type=pl.DeviceIdType.MESH)

    peer_w = [
        remote(w_gate, gate_w.at[1], peer_send.at[0], peer_recv.at[0], peer),
        remote(w_up, up_w.at[1], peer_send.at[1], peer_recv.at[1], peer),
        remote(w_down, down_w.at[1], peer_send.at[2], peer_recv.at[2], peer),
    ]

    def rows_of(t):
        return pl.ds(pl.multiple_of(t * ROWS, ROWS), ROWS)

    def mid_copy(d, s, t):
        return remote(result.at[s, d, rows_of(t)], mid_in.at[d, s, rows_of(t)],
                      mid_send.at[s, d, t], mid_recv.at[s, d, t], next_dev[d])

    def near_copy(d, t, slot):
        return remote(stage.at[slot, d], near_in.at[d, rows_of(t)], stage_send.at[slot, d], near_recv.at[d, t], next_dev[d])

    def far_copy(d, t, slot):
        return remote(stage.at[slot, d], far_in.at[d, rows_of(t)], stage_send.at[slot, d], far_recv.at[d, t], next_dev[d])

    def last_copy(d, i):
        here = pl.ds((tiles - 1) * ROWS + i * SUB, SUB)
        return remote(stage.at[last_place, d, pl.ds(i * SUB, SUB)], far_in.at[d, here],
                      last_send.at[d, i], last_recv.at[d, i], next_dev[d])

    def piece_copy(d, i, j):
        here, cols = pl.ds(i * FIRST, FIRST), pl.ds(j * YCOLS, YCOLS)
        return remote(result.at[0, d, here, cols], mid_in.at[d, 0, here, cols],
                      piece_send.at[d, i, j], piece_recv.at[d, i, j], next_dev[d])

    pieces = [(d, i, j) for i in range(ROWS // FIRST) for j in range(width // YCOLS) for d in (RIGHT, LEFT)]

    def make_hidden(slot, s, piece=None):
        rows = pl.ds(0, 2 * ROWS) if piece is None else pl.ds(piece * 2 * FIRST, 2 * FIRST)

        def chunk(j, _):
            if piece == 0:
                wait_load(j)
            cols = pl.ds(pl.multiple_of(j * WCOLS, WCOLS), WCOLS)
            x = x_tile[slot, rows]
            gate = jnp.dot(x, gate_w[s, :, cols], preferred_element_type=jnp.float32)
            up = jnp.dot(x, up_w[s, :, cols], preferred_element_type=jnp.float32)
            hidden[s, rows, cols] = (jax.nn.silu(gate) * up).astype(jnp.bfloat16)
            return 0
        if piece == 0:
            for j in range(depth // WCOLS):
                chunk(j, 0)
        else:
            lax.fori_loop(0, depth // WCOLS, chunk, 0)

    def part(s, cols, rows=pl.ds(0, 2 * ROWS)):
        return jnp.dot(hidden[s, rows], down_w[s, :, cols], preferred_element_type=jnp.float32).astype(jnp.bfloat16)

    def both(slot, store):
        make_hidden(slot, 0)
        make_hidden(slot, 1)

        def chunk(j, _):
            cols = pl.ds(pl.multiple_of(j * YCOLS, YCOLS), YCOLS)
            store(cols, part(0, cols).astype(jnp.float32) + part(1, cols).astype(jnp.float32))
            return 0
        lax.fori_loop(0, width // YCOLS, chunk, 0)

    def next_x(stg, t, slot):
        @pl.when(t < tiles - 1)
        def _():
            start_x(stg, t + 1, 1 - slot)
        if stg < 4:
            @pl.when(t == tiles - 1)
            def _():
                start_x(stg + 1, 0, 1 - slot)

    def mid_step(t, s):
            slot = lax.rem(t, 2)
            next_x(s, t, slot)
            wait_x(s, t, slot)
            make_hidden(slot, s)

            def chunk(j, _):
                cols = pl.ds(pl.multiple_of(j * YCOLS, YCOLS), YCOLS)
                y = part(s, cols)
                result[s, RIGHT, rows_of(t), cols] = y[:ROWS]
                result[s, LEFT, rows_of(t), cols] = y[ROWS:]
                return 0
            lax.fori_loop(0, width // YCOLS, chunk, 0)
            for d in (RIGHT, LEFT):
                mid_copy(d, s, t).start()

    for i in range(ROWS // FIRST):
        for cp in piece_copies(i):
            cp.wait()
        make_hidden(0, 0, piece=i)
        if i == 0:
            pl.semaphore_wait(barrier, 3)

        def piece_chunk(j, i=i):
            if i == 0:
                wait_load(depth // WCOLS + j)
            cols = pl.ds(pl.multiple_of(j * YCOLS, YCOLS), YCOLS)
            y = part(0, cols, pl.ds(i * 2 * FIRST, 2 * FIRST))
            for d in (RIGHT, LEFT):
                result[0, d, pl.ds(i * FIRST, FIRST), cols] = y[d * FIRST:(d + 1) * FIRST]
            for d in (RIGHT, LEFT):
                piece_copy(d, i, j).start()
        for j in range(width // YCOLS):
            piece_chunk(j)
        if i == 0:
            own_gain.start()
            for cp in peer_w:
                cp.start()
            start_x(0, 1, 1)

    def mid_loop(s, t0):
        def step(t, _):
            mid_step(t, s)
            return 0
        lax.fori_loop(t0, tiles, step, 0)

    mid_loop(0, 1)
    for cp in peer_w:
        cp.wait_recv()
    mid_loop(1, 0)

    def near_step(t, _):
        slot, place = lax.rem(t, 2), lax.rem(t, SLOTS)
        next_x(2, t, slot)
        wait_x(2, t, slot)

        @pl.when(t >= SLOTS)
        def _():
            for d in (RIGHT, LEFT):
                near_copy(d, t - SLOTS, place).wait_send()

        def store(cols, y):
            stage[place, RIGHT, :, cols] = y[:ROWS]
            stage[place, LEFT, :, cols] = y[ROWS:]
        both(slot, store)
        for d in (RIGHT, LEFT):
            near_copy(d, t, place).start()
        return 0
    lax.fori_loop(0, tiles, near_step, 0)

    def mid_loads(t):
        return [pltpu.make_async_copy(mid_in.at[d, s, rows_of(t)], mid_tile.at[d, s], mid_sem.at[d, s])
                for d in (RIGHT, LEFT) for s in (0, 1)]

    def far_step(t, _):
        slot, place = lax.rem(t, 2), lax.rem(t + tiles, SLOTS)
        next_x(3, t, slot)
        wait_x(3, t, slot)
        for d in (RIGHT, LEFT):
            near_copy(d, t, place).wait_send()

        def store(cols, y):
            stage[place, RIGHT, :, cols] = y[:ROWS]
            stage[place, LEFT, :, cols] = y[ROWS:]
        both(slot, store)
        for d in (RIGHT, LEFT):
            mid_copy(d, 1, t).wait_recv()

        @pl.when(t == 0)
        def _():
            for piece in pieces:
                piece_copy(*piece).wait_recv()

        @pl.when(t > 0)
        def _():
            for d in (RIGHT, LEFT):
                mid_copy(d, 0, t).wait_recv()
        for cp in mid_loads(t):
            cp.start()
        for cp in mid_loads(t):
            cp.wait()

        def add(j, _):
            r = pl.ds(pl.multiple_of(j * 16, 16), 16)
            for d in (RIGHT, LEFT):
                stage[place, d, r] += mid_tile[d, 0, r].astype(jnp.float32) + mid_tile[d, 1, r].astype(jnp.float32)
            return 0
        lax.fori_loop(0, ROWS // 16, add, 0)

        @pl.when(t < tiles - 1)
        def _():
            for d in (RIGHT, LEFT):
                far_copy(d, t, place).start()

        @pl.when(t == tiles - 1)
        def _():
            for i in range(ROWS // SUB):
                for d in (RIGHT, LEFT):
                    last_copy(d, i).start()
        return 0
    lax.fori_loop(0, tiles, far_step, 0)

    def own_loads(t):
        out = []
        for h in (0, 1):
            row = pl.multiple_of(h * half + t * ROWS, ROWS)
            out.append(pltpu.make_async_copy(near_in.at[1 - h, rows_of(t)], extra.at[h], extra_sem.at[h]))
            out.append(pltpu.make_async_copy(residual.at[pl.ds(row, ROWS)], res_tile.at[h], res_sem.at[h]))
        return out

    def own_step(t, _):
        slot = lax.rem(t, 2)
        next_x(4, t, slot)
        wait_x(4, t, slot)

        def store(cols, y):
            acc[0, rows_of(t), cols] = y[:ROWS]
            acc[1, rows_of(t), cols] = y[ROWS:]
        both(slot, store)
        for d in (RIGHT, LEFT):
            near_copy(d, t, 0).wait_recv()
        for cp in own_loads(t):
            cp.start()
        for cp in own_loads(t):
            cp.wait()

        def add(j, _):
            r = pl.ds(pl.multiple_of(j * 16, 16), 16)
            here = pl.ds(pl.multiple_of(t * ROWS + j * 16, 16), 16)
            for h in (0, 1):
                acc[h, here] += extra[h, r] + res_tile[h, r].astype(jnp.float32)
            return 0
        lax.fori_loop(0, ROWS // 16, add, 0)
        return 0
    lax.fori_loop(0, tiles, own_step, 0)

    for cp in peer_w:
        cp.wait_send()

    for piece in pieces:
        piece_copy(*piece).wait_send()

    def drain(t, _):
        for d in (RIGHT, LEFT):
            mid_copy(d, 1, t).wait_send()

        @pl.when(t > 0)
        def _():
            for d in (RIGHT, LEFT):
                mid_copy(d, 0, t).wait_send()
        return 0
    lax.fori_loop(0, tiles, drain, 0)
    own_gain.wait()

    def finish(row):
        for h in (0, 1):
            here = pl.ds(row, 16)
            value = acc[h, here] + far_in[h, here]
            mean_sq = jnp.mean(value * value, axis=-1, keepdims=True)
            result[0, h, here] = value.astype(jnp.bfloat16)
            result[1, h, here] = (value * lax.rsqrt(mean_sq + EPS) * gain[...]).astype(jnp.bfloat16)

    def last_step(t, _):
        for d in (RIGHT, LEFT):
            far_copy(d, t, 0).wait_recv()

        def rows16(j, _):
            finish(pl.multiple_of(t * ROWS + j * 16, 16))
            return 0
        lax.fori_loop(0, ROWS // 16, rows16, 0)
        return 0
    lax.fori_loop(0, tiles - 1, last_step, 0)

    for place in range(SLOTS):
        if place != last_place:
            for d in (RIGHT, LEFT):
                far_copy(d, 0, place).wait_send()

    for i in range(ROWS // SUB):
        for d in (RIGHT, LEFT):
            last_copy(d, i).wait_recv()
        for j in range(SUB // 16):
            finish((tiles - 1) * ROWS + i * SUB + j * 16)
    for i in range(ROWS // SUB):
        for d in (RIGHT, LEFT):
            last_copy(d, i).wait_send()


def write_kernel(result, h_out, normed, sem):
    half = result.shape[2]
    copies = [
        pltpu.make_async_copy(result.at[i, h], out.at[pl.ds(h * half, half)], sem.at[i, h])
        for i, out in enumerate((h_out, normed)) for h in (0, 1)]
    for cp in copies:
        cp.start()
    for cp in copies:
        cp.wait()


def solution(mesh):
    n = mesh.shape["tp"]

    def local_block(x_in, w_gate, w_up, w_down, residual, norm_gain):
        rows, width = residual.shape
        depth = w_gate.shape[1]
        half = rows // 2
        tiles = half // ROWS
        f32, bf16 = jnp.float32, jnp.bfloat16
        dma = pltpu.SemaphoreType.DMA
        any_space = pl.BlockSpec(memory_space=pl.ANY)
        result, _, _ = pl.pallas_call(
            functools.partial(ring_kernel, n),
            out_shape=(
                pltpu.VMEM((2, 2, half, width), bf16),
                jax.ShapeDtypeStruct((2, 2, half, width), bf16),
                jax.ShapeDtypeStruct((2, half, width), f32),
            ),
            in_specs=[any_space] * 6,
            out_specs=(pl.BlockSpec(memory_space=pltpu.VMEM), any_space, any_space),
            scratch_shapes=[
                pltpu.VMEM((2,) + w_gate.shape, bf16),
                pltpu.VMEM((2,) + w_up.shape, bf16),
                pltpu.VMEM((2,) + w_down.shape, bf16),
                pltpu.VMEM((2, 2 * ROWS, width), bf16),
                pltpu.VMEM((2, 2 * ROWS, depth), bf16),
                pltpu.VMEM((SLOTS, 2, ROWS, width), f32),
                pltpu.VMEM((2, half, width), f32),
                pltpu.VMEM((2, half, width), f32),
                pltpu.VMEM((2, ROWS, width), f32),
                pltpu.VMEM((2, 2, ROWS, width), bf16),
                pltpu.VMEM((2, ROWS, width), bf16),
                pltpu.VMEM((1, width), f32),
                dma((depth // WCOLS,)), dma((depth // WCOLS,)), dma((width // YCOLS,)), dma((3,)), dma((3,)),
                dma((2, 2)),
                dma((2, 2, tiles)), dma((2, 2, tiles)),
                dma((SLOTS, 2)), dma((2, tiles)), dma((2, tiles)),
                dma((2, ROWS // SUB)), dma((2, ROWS // SUB)),
                dma((2,)), dma((2, 2)), dma((2,)), dma(()),
                dma((ROWS // FIRST, 2)), dma((2, ROWS // FIRST, width // YCOLS)), dma((2, ROWS // FIRST, width // YCOLS)),
            ],
            compiler_params=pltpu.CompilerParams(
                collective_id=0, has_side_effects=True, vmem_limit_bytes=55 * 2**20),
            name="ring",
        )(x_in, w_gate, w_up, w_down, residual, norm_gain.reshape(1, width))
        return pl.pallas_call(
            write_kernel,
            out_shape=(jax.ShapeDtypeStruct((rows, width), bf16),) * 2,
            in_specs=[pl.BlockSpec(memory_space=pltpu.VMEM)],
            out_specs=(any_space, any_space),
            scratch_shapes=[dma((2, 2))],
            compiler_params=pltpu.CompilerParams(vmem_limit_bytes=2**20),
            name="write",
        )(pltpu.with_memory_space_constraint(result, pltpu.VMEM))

    row_spec = P(("data", "tp"), None)
    return jax.shard_map(local_block, mesh=mesh, in_specs=(P("data", None), P(None, "tp"), P(None, "tp"), P("tp", None), row_spec, P(None)), out_specs=(row_spec, row_spec), check_vma=False)
```

```python
import functools

import jax
import jax.numpy as jnp
from jax import lax
from jax.experimental import pallas as pl
from jax.experimental.pallas import tpu as pltpu
from jax.sharding import PartitionSpec as P

EPS = 1e-5
CORES = 2
ROWS = 128
FAR_SLOTS, NEAR_SLOTS = 3, 2
SUB = 32
FIRST = 64
WCOLS = 256
YCOLS = 512
AHEAD = 4
RIGHT, LEFT = 0, 1
VMEM_LIMIT = 58_500_000


def ring_kernel(
    n, x_in, w_gate, w_up, w_down, residual, norm_gain, result, y_in, g_in, down_in,
    gate_w, up_w, down_w, x_tile, hidden, near_y, near_g, stage, far_in, acc, y_tile, g_tile, gain,
    gate_sem, up_sem, down_sem, gain_sem, x_sem, piece_sem, tile_sem, res_sem,
    peer_send, peer_recv, first_send, first_recv, mid_send, mid_recv, near_send, near_recv, far_send, far_recv,
    last_send, last_recv, whole_send, whole_recv, swap_send, swap_recv, load_sem,
):
    me = lax.axis_index("tp")
    chips = n // CORES
    chip, core = me // CORES, lax.rem(me, CORES)
    own_rows = residual.shape[0]
    half = own_rows // 2
    tiles = half // ROWS
    depth, width = w_gate.shape[1], w_down.shape[1]
    half_depth = depth // 2

    def device(c, k):
        return {"tp": lax.rem(c + chips, chips) * CORES + k}

    right, left, peer = device(chip + 1, core), device(chip - 1, core), device(chip, 1 - core)
    next_dev = (right, left)
    last = tiles - 1
    last_place = last % FAR_SLOTS

    def x_copies(stg, t, slot):
        (c0, h0), (c1, h1) = (
            ((chip + 2, 0), (chip + 2, 1)),
            ((chip + 2, 0), (chip + 2, 1)),
            ((chip + 1, 1), (chip - 1, 0)),
            ((chip + 1, 0), (chip - 1, 1)),
            ((chip, 0), (chip, 1)),
        )[stg]
        out = []
        for d, (c, h) in enumerate(((c0, h0), (c1, h1))):
            c = lax.rem(c + chips, chips)
            row = pl.multiple_of((c * CORES + core) * own_rows + h * half + t * ROWS, ROWS)
            out.append(pltpu.make_async_copy(
                x_in.at[pl.ds(row, ROWS)], x_tile.at[slot, pl.ds(d * ROWS, ROWS)], x_sem.at[slot, d]))
        return out

    def start_x(stg, t, slot):
        for cp in x_copies(stg, t, slot):
            cp.start()

    def wait_x(stg, t, slot):
        for cp in x_copies(stg, t, slot):
            cp.wait()

    def piece_copies(i):
        out = []
        for d in (RIGHT, LEFT):
            row = pl.multiple_of((lax.rem(chip + 2, chips) * CORES + core) * own_rows + d * half + i * FIRST, FIRST)
            out.append(pltpu.make_async_copy(
                x_in.at[pl.ds(row, FIRST)], x_tile.at[0, pl.ds((2 * i + d) * FIRST, FIRST)], piece_sem.at[i, d]))
        return out

    def own_cols(j):
        cols = pl.ds(pl.multiple_of(j * WCOLS, WCOLS), WCOLS)
        return [
            pltpu.make_async_copy(w_gate.at[:, cols], gate_w.at[core, :, cols], gate_sem.at[j]),
            pltpu.make_async_copy(w_up.at[:, cols], up_w.at[core, :, cols], up_sem.at[j]),
        ]

    def own_down(j):
        cols = pl.ds(pl.multiple_of(j * YCOLS, YCOLS), YCOLS)
        return pltpu.make_async_copy(w_down.at[:, cols], down_w.at[core, :, cols], down_sem.at[j])

    own_gain = pltpu.make_async_copy(norm_gain, gain, gain_sem)
    loads = [own_cols(j) for j in range(depth // WCOLS)] + [[own_down(j)] for j in range(width // YCOLS)]

    def start_load(i):
        for cp in loads[i] if i < len(loads) else ():
            cp.start()

    def wait_load(i):
        for cp in loads[i]:
            cp.wait()
        start_load(i + AHEAD)

    for cp in piece_copies(0):
        cp.start()
    for i in range(AHEAD):
        start_load(i)
    for k in range(1, ROWS // FIRST):
        for cp in piece_copies(k):
            cp.start()

    barrier = pltpu.get_barrier_semaphore()
    for dev in (peer, left, right):
        pl.semaphore_signal(barrier, inc=1, device_id=dev, device_id_type=pl.DeviceIdType.MESH)

    def remote(src, dst, send, recv, dev):
        return pltpu.make_async_remote_copy(
            src_ref=src, dst_ref=dst, send_sem=send, recv_sem=recv, device_id=dev, device_id_type=pl.DeviceIdType.MESH)

    peer_w = [
        remote(w, dst.at[core], peer_send.at[i], peer_recv.at[i], peer)
        for i, (w, dst) in enumerate(((w_gate, gate_w), (w_up, up_w), (w_down, down_w)))]
    my_half = pl.ds(pl.multiple_of(core * half_depth, half_depth), half_depth)

    def down_copy(d, src):
        return remote(src, down_in.at[d, my_half], whole_send.at[d], whole_recv.at[d], next_dev[d])

    def swap_copy(d):
        return remote(down_in.at[d, my_half], down_in.at[d, my_half], swap_send.at[d], swap_recv.at[d], peer)

    @pl.when(core == 0)
    def _():
        pl.semaphore_wait(barrier, 3)
        for d in (RIGHT, LEFT):
            down_copy(d, w_down.at[pl.ds(0, half_depth)]).start()

    def rows_of(t):
        return pl.ds(pl.multiple_of(t * ROWS, ROWS), ROWS)

    def mid_y(d, t):
        return remote(result.at[1, d, rows_of(t)], y_in.at[0, d, rows_of(t)], mid_send.at[1, d, t], mid_recv.at[1, d, t], next_dev[d])

    def mid_g(d, t):
        return remote(result.at[0, d, rows_of(t), pl.ds(0, depth)], g_in.at[0, d, rows_of(t)],
                      mid_send.at[0, d, t], mid_recv.at[0, d, t], next_dev[d])

    def near_copies(d, t, place):
        return [
            remote(near_g.at[place, d], g_in.at[1, d, rows_of(t)], near_send.at[place, d, 0], near_recv.at[0, d, t], next_dev[d]),
            remote(near_y.at[place, d], y_in.at[1, d, rows_of(t)], near_send.at[place, d, 1], near_recv.at[1, d, t], next_dev[d]),
        ]

    def far_copy(d, t, place):
        return remote(stage.at[place, d], far_in.at[d, rows_of(t)], far_send.at[place, d], far_recv.at[d, t], next_dev[d])

    def last_copy(d, i):
        here = pl.ds(last * ROWS + i * SUB, SUB)
        return remote(stage.at[last_place, d, pl.ds(i * SUB, SUB)], far_in.at[d, here],
                      last_send.at[d, i], last_recv.at[d, i], next_dev[d])

    def piece_copy(d, i, j):
        here, cols = pl.ds(i * FIRST, FIRST), pl.ds(j * YCOLS, YCOLS)
        return remote(result.at[1, d, here, cols], y_in.at[0, d, here, cols],
                      first_send.at[d, i, j], first_recv.at[d, i, j], next_dev[d])

    pieces = [(d, i, j) for i in range(ROWS // FIRST) for j in range(width // YCOLS) for d in (RIGHT, LEFT)]

    def make_hidden(slot, s, piece=None):
        rows = pl.ds(0, 2 * ROWS) if piece is None else pl.ds(piece * 2 * FIRST, 2 * FIRST)

        def chunk(j, _):
            if piece == 0:
                wait_load(j)
            cols = pl.ds(pl.multiple_of(j * WCOLS, WCOLS), WCOLS)
            x = x_tile[slot, rows]
            gate = jnp.dot(x, gate_w[s, :, cols], preferred_element_type=jnp.float32)
            up = jnp.dot(x, up_w[s, :, cols], preferred_element_type=jnp.float32)
            hidden[s, rows, cols] = (jax.nn.silu(gate) * up).astype(jnp.bfloat16)
            return 0
        if piece == 0:
            for j in range(depth // WCOLS):
                chunk(j, 0)
        else:
            lax.fori_loop(0, depth // WCOLS, chunk, 0)

    def part(s, cols, rows=pl.ds(0, 2 * ROWS)):
        return jnp.dot(hidden[s, rows], down_w[s, :, cols], preferred_element_type=jnp.float32).astype(jnp.bfloat16)

    def both(slot, store):
        make_hidden(slot, 0)
        make_hidden(slot, 1)

        def chunk(j, _):
            cols = pl.ds(pl.multiple_of(j * YCOLS, YCOLS), YCOLS)
            store(cols, part(0, cols).astype(jnp.float32) + part(1, cols).astype(jnp.float32))
            return 0
        lax.fori_loop(0, width // YCOLS, chunk, 0)

    def start_pieces():
        for piece in pieces:
            piece_copy(*piece).start()

    for i in range(ROWS // FIRST):
        rows = pl.ds(i * 2 * FIRST, 2 * FIRST)
        for cp in piece_copies(i):
            cp.wait()
        make_hidden(0, core, piece=i)

        @pl.when(core == 1)
        def _(i=i, rows=rows):
            if i == 0:
                pl.semaphore_wait(barrier, 3)
            for j in range(width // YCOLS):
                if i == 0:
                    wait_load(depth // WCOLS + j)
                cols = pl.ds(j * YCOLS, YCOLS)
                y = part(1, cols, rows)
                for d in (RIGHT, LEFT):
                    result[1, d, pl.ds(i * FIRST, FIRST), cols] = y[d * FIRST:(d + 1) * FIRST]
                for d in (RIGHT, LEFT):
                    piece_copy(d, i, j).start()

        @pl.when(core == 0)
        def _(i=i):
            for j in range(width // YCOLS) if i == 0 else ():
                wait_load(depth // WCOLS + j)
            for d in (RIGHT, LEFT):
                result[0, d, pl.ds(i * FIRST, FIRST), pl.ds(0, depth)] = hidden[0, pl.ds((2 * i + d) * FIRST, FIRST)]
        if i == 0:
            own_gain.start()
            for cp in peer_w:
                cp.start()
            start_x(0, 1, 1)

    @pl.when(core == 0)
    def _():
        for d in (RIGHT, LEFT):
            mid_g(d, 0).start()

    def mid_step(stg, t, s):
        slot = lax.rem(t, 2)

        @pl.when(t < last)
        def _():
            start_x(stg, t + 1, 1 - slot)

        @pl.when(t == last)
        def _():
            start_x(stg + 1, 0, 1 - slot)
        wait_x(stg, t, slot)
        make_hidden(slot, s)

        @pl.when(s == 0)
        def _():
            for d in (RIGHT, LEFT):
                result[0, d, rows_of(t), pl.ds(0, depth)] = hidden[0, pl.ds(d * ROWS, ROWS)]
            for d in (RIGHT, LEFT):
                mid_g(d, t).start()

        @pl.when(s == 1)
        def _():
            def chunk(j, _):
                cols = pl.ds(pl.multiple_of(j * YCOLS, YCOLS), YCOLS)
                y = part(1, cols)
                for d in (RIGHT, LEFT):
                    result[1, d, rows_of(t), cols] = y[d * ROWS:(d + 1) * ROWS]
                return 0
            lax.fori_loop(0, width // YCOLS, chunk, 0)

            @pl.when(t == 0)
            def _():
                start_pieces()

            @pl.when(t > 0)
            def _():
                for d in (RIGHT, LEFT):
                    mid_y(d, t).start()

    def loop(t0, t1, step):
        def body(t, _):
            step(t)
            return 0
        lax.fori_loop(t0, t1, body, 0)

    loop(1, tiles, lambda t: mid_step(0, t, core))
    for cp in peer_w:
        cp.wait_recv()

    @pl.when(core == 1)
    def _():
        for d in (RIGHT, LEFT):
            down_copy(d, down_w.at[0, pl.ds(half_depth, half_depth)]).start()
    loop(0, tiles, lambda t: mid_step(1, t, 1 - core))

    def near_step(t):
        slot, place = lax.rem(t, 2), lax.rem(t, NEAR_SLOTS)

        for now, stg, nxt in ((0, 2, 1), (NEAR_SLOTS - 1, 4, 0), (NEAR_SLOTS, 2, NEAR_SLOTS + 1), (last, 3, 0)):
            @pl.when(t == now)
            def _(stg=stg, nxt=nxt):
                start_x(stg, nxt, 1 - slot)
        wait_x(2, t, slot)
        make_hidden(slot, 0)
        make_hidden(slot, 1)

        @pl.when(t >= NEAR_SLOTS)
        def _():
            for d in (RIGHT, LEFT):
                for cp in near_copies(d, t - NEAR_SLOTS, place):
                    cp.wait_send()
        for d in (RIGHT, LEFT):
            near_g[place, d] = hidden[0, pl.ds(d * ROWS, ROWS)]

        def chunk(j, _):
            cols = pl.ds(pl.multiple_of(j * YCOLS, YCOLS), YCOLS)
            y = part(1, cols)
            for d in (RIGHT, LEFT):
                near_y[place, d, :, cols] = y[d * ROWS:(d + 1) * ROWS]
            return 0
        lax.fori_loop(0, width // YCOLS, chunk, 0)
        for d in (RIGHT, LEFT):
            for cp in near_copies(d, t, place):
                cp.start()
    loop(0, NEAR_SLOTS, near_step)

    def own_step(t):
        slot = lax.rem(t, 2)

        @pl.when(t < last)
        def _():
            start_x(4, t + 1, 1 - slot)

        @pl.when(t == last)
        def _():
            start_x(2, NEAR_SLOTS, 1 - slot)
        wait_x(4, t, slot)
        res_copies = [pltpu.make_async_copy(
            residual.at[pl.ds(pl.multiple_of(h * half + t * ROWS, ROWS), ROWS)], y_tile.at[h], res_sem.at[h]) for h in (0, 1)]
        for cp in res_copies:
            cp.start()
        for cp in res_copies:
            cp.wait()

        def store(cols, y):
            for h in (0, 1):
                acc[h, rows_of(t), cols] = y[h * ROWS:(h + 1) * ROWS] + y_tile[h, :, cols].astype(jnp.float32)
        both(slot, store)

    loop(0, tiles, own_step)

    for d in (RIGHT, LEFT):
        down_copy(d, w_down.at[pl.ds(0, half_depth)]).wait_recv()
        swap_copy(d).start()
    for piece in pieces:
        piece_copy(*piece).wait_send()
    loop(0, tiles, lambda t: [mid_g(d, t).wait_send() for d in (RIGHT, LEFT)])
    loop(1, tiles, lambda t: [mid_y(d, t).wait_send() for d in (RIGHT, LEFT)])
    for d in (RIGHT, LEFT):
        swap_copy(d).wait_recv()
    loads = [pltpu.make_async_copy(down_in.at[d, pl.ds(h * half_depth, half_depth)], result.at[d, h], load_sem.at[d, h])
             for d in (RIGHT, LEFT) for h in (0, 1)]
    for cp in loads:
        cp.start()
    for cp in loads:
        cp.wait()

    loop(NEAR_SLOTS, tiles, near_step)


    def load_terms(kind, t):
        cps = []
        for d in (RIGHT, LEFT):
            cps.append(pltpu.make_async_copy(y_in.at[kind, d, rows_of(t)], y_tile.at[d], tile_sem.at[1, d]))
            cps.append(pltpu.make_async_copy(g_in.at[kind, d, rows_of(t)], g_tile.at[d], tile_sem.at[0, d]))
        return cps

    def term(d, cols):
        w = result[d, :, :, cols].reshape(depth, YCOLS)
        y = jnp.dot(g_tile[d], w, preferred_element_type=jnp.float32).astype(jnp.bfloat16)
        return y.astype(jnp.float32) + y_tile[d, :, cols].astype(jnp.float32)

    def far_tile(t, slot, place):
        wait_x(3, t, slot)

        def store(cols, y):
            for d in (RIGHT, LEFT):
                stage[place, d, :, cols] = y[d * ROWS:(d + 1) * ROWS]
        both(slot, store)
        for d in (RIGHT, LEFT):
            mid_g(d, t).wait_recv()

        @pl.when(t == 0)
        def _():
            for piece in pieces:
                piece_copy(*piece).wait_recv()

        @pl.when(t > 0)
        def _():
            for d in (RIGHT, LEFT):
                mid_y(d, t).wait_recv()
        for cp in load_terms(0, t):
            cp.start()
        for cp in load_terms(0, t):
            cp.wait()

        def chunk(j, _):
            cols = pl.ds(pl.multiple_of(j * YCOLS, YCOLS), YCOLS)
            for d in (RIGHT, LEFT):
                stage[place, d, :, cols] += term(d, cols)
            return 0
        lax.fori_loop(0, width // YCOLS, chunk, 0)

    def far_step(t):
        slot, place = lax.rem(t, 2), lax.rem(t, FAR_SLOTS)

        @pl.when(t < last)
        def _():
            start_x(3, t + 1, 1 - slot)

        @pl.when(t >= FAR_SLOTS)
        def _():
            for d in (RIGHT, LEFT):
                far_copy(d, t - FAR_SLOTS, place).wait_send()
        far_tile(t, slot, place)

        @pl.when(t < last)
        def _():
            for d in (RIGHT, LEFT):
                far_copy(d, t, place).start()

        @pl.when(t == last)
        def _():
            for i in range(ROWS // SUB):
                for d in (RIGHT, LEFT):
                    last_copy(d, i).start()
    loop(0, tiles, far_step)

    def own_terms(t):
        for d in (RIGHT, LEFT):
            for cp in near_copies(d, t, 0):
                cp.wait_recv()
        for cp in load_terms(1, t):
            cp.start()
        for cp in load_terms(1, t):
            cp.wait()

        def chunk(j, _):
            cols = pl.ds(pl.multiple_of(j * YCOLS, YCOLS), YCOLS)
            for h in (0, 1):
                acc[h, rows_of(t), cols] += term(1 - h, cols)
            return 0
        lax.fori_loop(0, width // YCOLS, chunk, 0)

    loop(0, tiles, own_terms)

    for cp in peer_w:
        cp.wait_send()
    for d in (RIGHT, LEFT):
        down_copy(d, w_down.at[pl.ds(0, half_depth)]).wait_send()
        swap_copy(d).wait_send()
        for place in range(NEAR_SLOTS):
            for cp in near_copies(d, 0, place):
                cp.wait_send()
    own_gain.wait()

    def finish(row):
        for h in (0, 1):
            here = pl.ds(row, 16)
            value = acc[h, here] + far_in[h, here]
            mean_sq = jnp.mean(value * value, axis=-1, keepdims=True)
            result[0, h, here] = value.astype(jnp.bfloat16)
            result[1, h, here] = (value * lax.rsqrt(mean_sq + EPS) * gain[...]).astype(jnp.bfloat16)

    def last_step(t):
        for d in (RIGHT, LEFT):
            far_copy(d, t, 0).wait_recv()
        loop(0, ROWS // 16, lambda j: finish(pl.multiple_of(t * ROWS + j * 16, 16)))
    loop(0, last, last_step)

    for place in range(FAR_SLOTS):
        if place != last_place:
            for d in (RIGHT, LEFT):
                far_copy(d, 0, place).wait_send()

    for i in range(ROWS // SUB):
        for d in (RIGHT, LEFT):
            last_copy(d, i).wait_recv()
        for j in range(SUB // 16):
            finish(last * ROWS + i * SUB + j * 16)
    for i in range(ROWS // SUB):
        for d in (RIGHT, LEFT):
            last_copy(d, i).wait_send()


def write_kernel(result, h_out, normed, sem):
    half = result.shape[2]
    copies = [
        pltpu.make_async_copy(result.at[i, h], out.at[pl.ds(h * half, half)], sem.at[i, h])
        for i, out in enumerate((h_out, normed)) for h in (0, 1)]
    for cp in copies:
        cp.start()
    for cp in copies:
        cp.wait()


def solution(mesh):
    n = mesh.shape["tp"]

    def local_block(x_in, w_gate, w_up, w_down, residual, norm_gain):
        rows, width = residual.shape
        depth = w_gate.shape[1]
        half = rows // 2
        tiles = half // ROWS
        f32, bf16 = jnp.float32, jnp.bfloat16
        dma = pltpu.SemaphoreType.DMA
        any_space = pl.BlockSpec(memory_space=pl.ANY)
        result, _, _, _ = pl.pallas_call(
            functools.partial(ring_kernel, n),
            out_shape=(
                pltpu.VMEM((2, 2, half, width), bf16),
                jax.ShapeDtypeStruct((2, 2, half, width), bf16),
                jax.ShapeDtypeStruct((2, 2, half, depth), bf16),
                jax.ShapeDtypeStruct((2, depth, width), bf16),
            ),
            in_specs=[any_space] * 6,
            out_specs=(pl.BlockSpec(memory_space=pltpu.VMEM),) + (any_space,) * 3,
            scratch_shapes=[
                pltpu.VMEM((2,) + w_gate.shape, bf16),
                pltpu.VMEM((2,) + w_up.shape, bf16),
                pltpu.VMEM((2,) + w_down.shape, bf16),
                pltpu.VMEM((2, 2 * ROWS, width), bf16),
                pltpu.VMEM((2, 2 * ROWS, depth), bf16),
                pltpu.VMEM((NEAR_SLOTS, 2, ROWS, width), bf16),
                pltpu.VMEM((NEAR_SLOTS, 2, ROWS, depth), bf16),
                pltpu.VMEM((FAR_SLOTS, 2, ROWS, width), f32),
                pltpu.VMEM((2, half, width), f32),
                pltpu.VMEM((2, half, width), f32),
                pltpu.VMEM((2, ROWS, width), bf16),
                pltpu.VMEM((2, ROWS, depth), bf16),
                pltpu.VMEM((1, width), f32),
                dma((depth // WCOLS,)), dma((depth // WCOLS,)), dma((width // YCOLS,)), dma(()), dma((2, 2)),
                dma((ROWS // FIRST, 2)), dma((2, 2)), dma((2,)),
                dma((3,)), dma((3,)),
                dma((2, ROWS // FIRST, width // YCOLS)), dma((2, ROWS // FIRST, width // YCOLS)),
                dma((2, 2, tiles)), dma((2, 2, tiles)),
                dma((NEAR_SLOTS, 2, 2)), dma((2, 2, tiles)),
                dma((FAR_SLOTS, 2)), dma((2, tiles)),
                dma((2, ROWS // SUB)), dma((2, ROWS // SUB)),
                dma((2,)), dma((2,)), dma((2,)), dma((2,)), dma((2, 2)),
            ],
            compiler_params=pltpu.CompilerParams(
                collective_id=0, has_side_effects=True, vmem_limit_bytes=VMEM_LIMIT),
            name="ring",
        )(x_in, w_gate, w_up, w_down, residual, norm_gain.reshape(1, width))
        return pl.pallas_call(
            write_kernel,
            out_shape=(jax.ShapeDtypeStruct((rows, width), bf16),) * 2,
            in_specs=[pl.BlockSpec(memory_space=pltpu.VMEM)],
            out_specs=(any_space, any_space),
            scratch_shapes=[dma((2, 2))],
            compiler_params=pltpu.CompilerParams(vmem_limit_bytes=2**20),
            name="write",
        )(pltpu.with_memory_space_constraint(result, pltpu.VMEM))

    row_spec = P(("data", "tp"), None)
    return jax.shard_map(local_block, mesh=mesh, in_specs=(P("data", None), P(None, "tp"), P(None, "tp"), P("tp", None), row_spec, P(None)), out_specs=(row_spec, row_spec), check_vma=False)
```

```python
import functools

import jax
import jax.numpy as jnp
from jax import lax
from jax.experimental import pallas as pl
from jax.experimental.pallas import tpu as pltpu
from jax.sharding import PartitionSpec as P

EPS = 1e-5
CORES = 2
ROWS = 128
FAR_SLOTS, NEAR_SLOTS = 3, 2
SUB = 32
FIRST = 64
WCOLS = 256
YCOLS = 512
AHEAD = 4
RIGHT, LEFT = 0, 1
VMEM_LIMIT = 58_500_000


def ring_kernel(
    n, x_in, w_gate, w_up, w_down, residual, norm_gain, result, y_in, g_in, down_in,
    gate_w, up_w, down_w, x_tile, hidden, near_y, near_g, stage, far_in, acc, y_tile, g_tile, gain,
    gate_sem, up_sem, down_sem, gain_sem, x_sem, piece_sem, tile_sem, res_sem,
    peer_send, peer_recv, first_send, first_recv, mid_send, mid_recv, near_send, near_recv, far_send, far_recv,
    last_send, last_recv, whole_send, whole_recv, swap_send, swap_recv, load_sem,
):
    me = lax.axis_index("tp")
    chips = n // CORES
    chip, core = me // CORES, CORES - 1 - lax.rem(me, CORES)
    own_rows = residual.shape[0]
    half = own_rows // 2
    tiles = half // ROWS
    depth, width = w_gate.shape[1], w_down.shape[1]
    half_depth = depth // 2

    def position(c, k):
        return lax.rem(c + chips, chips) * CORES + CORES - 1 - k

    def device(c, k):
        return {"tp": position(c, k)}

    right, left, peer = device(chip + 1, core), device(chip - 1, core), device(chip, 1 - core)
    next_dev = (right, left)
    last = tiles - 1
    last_place = last % FAR_SLOTS

    barrier = pltpu.get_barrier_semaphore()
    for dev in (peer, left, right):
        pl.semaphore_signal(barrier, inc=1, device_id=dev, device_id_type=pl.DeviceIdType.MESH)

    def remote(src, dst, send, recv, dev):
        return pltpu.make_async_remote_copy(
            src_ref=src, dst_ref=dst, send_sem=send, recv_sem=recv, device_id=dev, device_id_type=pl.DeviceIdType.MESH)

    peer_w = [
        remote(w, dst.at[core], peer_send.at[i], peer_recv.at[i], peer)
        for i, (w, dst) in enumerate(((w_gate, gate_w), (w_up, up_w), (w_down, down_w)))]
    my_half = pl.ds(pl.multiple_of(core * half_depth, half_depth), half_depth)

    def down_copy(d, src):
        return remote(src, down_in.at[d, my_half], whole_send.at[d], whole_recv.at[d], next_dev[d])

    def swap_copy(d):
        return remote(down_in.at[d, my_half], down_in.at[d, my_half], swap_send.at[d], swap_recv.at[d], peer)

    @pl.when(core == 0)
    def _():
        pl.semaphore_wait(barrier, 3)
        for d in (RIGHT, LEFT):
            down_copy(d, w_down.at[pl.ds(0, half_depth)]).start()

    def x_copies(stg, t, slot):
        (c0, h0), (c1, h1) = (
            ((chip + 2, 0), (chip + 2, 1)),
            ((chip + 2, 0), (chip + 2, 1)),
            ((chip + 1, 1), (chip - 1, 0)),
            ((chip + 1, 0), (chip - 1, 1)),
            ((chip, 0), (chip, 1)),
        )[stg]
        out = []
        for d, (c, h) in enumerate(((c0, h0), (c1, h1))):
            row = pl.multiple_of(position(c, core) * own_rows + h * half + t * ROWS, ROWS)
            out.append(pltpu.make_async_copy(
                x_in.at[pl.ds(row, ROWS)], x_tile.at[slot, pl.ds(d * ROWS, ROWS)], x_sem.at[slot, d]))
        return out

    def start_x(stg, t, slot):
        for cp in x_copies(stg, t, slot):
            cp.start()

    def wait_x(stg, t, slot):
        for cp in x_copies(stg, t, slot):
            cp.wait()

    def piece_copies(i):
        out = []
        for d in (RIGHT, LEFT):
            row = pl.multiple_of(position(chip + 2, core) * own_rows + d * half + i * FIRST, FIRST)
            out.append(pltpu.make_async_copy(
                x_in.at[pl.ds(row, FIRST)], x_tile.at[0, pl.ds((2 * i + d) * FIRST, FIRST)], piece_sem.at[i, d]))
        return out

    def own_cols(j):
        cols = pl.ds(pl.multiple_of(j * WCOLS, WCOLS), WCOLS)
        return [
            pltpu.make_async_copy(w_gate.at[:, cols], gate_w.at[core, :, cols], gate_sem.at[j]),
            pltpu.make_async_copy(w_up.at[:, cols], up_w.at[core, :, cols], up_sem.at[j]),
        ]

    def own_down(j):
        cols = pl.ds(pl.multiple_of(j * YCOLS, YCOLS), YCOLS)
        return pltpu.make_async_copy(w_down.at[:, cols], down_w.at[core, :, cols], down_sem.at[j])

    own_gain = pltpu.make_async_copy(norm_gain, gain, gain_sem)
    loads = [own_cols(j) for j in range(depth // WCOLS)] + [[own_down(j)] for j in range(width // YCOLS)]

    def start_load(i):
        for cp in loads[i] if i < len(loads) else ():
            cp.start()

    def wait_load(i):
        for cp in loads[i]:
            cp.wait()
        start_load(i + AHEAD)

    for cp in piece_copies(0):
        cp.start()
    for i in range(AHEAD):
        start_load(i)
    for k in range(1, ROWS // FIRST):
        for cp in piece_copies(k):
            cp.start()

    def rows_of(t):
        return pl.ds(pl.multiple_of(t * ROWS, ROWS), ROWS)

    def mid_y(d, t):
        return remote(result.at[1, d, rows_of(t)], y_in.at[0, d, rows_of(t)], mid_send.at[1, d, t], mid_recv.at[1, d, t], next_dev[d])

    def mid_g(d, t):
        return remote(result.at[0, d, rows_of(t), pl.ds(0, depth)], g_in.at[0, d, rows_of(t)],
                      mid_send.at[0, d, t], mid_recv.at[0, d, t], next_dev[d])

    def near_copies(d, t, place):
        return [
            remote(near_g.at[place, d], g_in.at[1, d, rows_of(t)], near_send.at[place, d, 0], near_recv.at[0, d, t], next_dev[d]),
            remote(near_y.at[place, d], y_in.at[1, d, rows_of(t)], near_send.at[place, d, 1], near_recv.at[1, d, t], next_dev[d]),
        ]

    def far_copy(d, t, place):
        return remote(stage.at[place, d], far_in.at[d, rows_of(t)], far_send.at[place, d], far_recv.at[d, t], next_dev[d])

    def last_copy(d, i):
        here = pl.ds(last * ROWS + i * SUB, SUB)
        return remote(stage.at[last_place, d, pl.ds(i * SUB, SUB)], far_in.at[d, here],
                      last_send.at[d, i], last_recv.at[d, i], next_dev[d])

    def piece_copy(d, i, j):
        here, cols = pl.ds(i * FIRST, FIRST), pl.ds(j * YCOLS, YCOLS)
        return remote(result.at[1, d, here, cols], y_in.at[0, d, here, cols],
                      first_send.at[d, i, j], first_recv.at[d, i, j], next_dev[d])

    pieces = [(d, i, j) for i in range(ROWS // FIRST) for j in range(width // YCOLS) for d in (RIGHT, LEFT)]

    def make_hidden(slot, s, piece=None):
        rows = pl.ds(0, 2 * ROWS) if piece is None else pl.ds(piece * 2 * FIRST, 2 * FIRST)

        def chunk(j, _):
            if piece == 0:
                wait_load(j)
            cols = pl.ds(pl.multiple_of(j * WCOLS, WCOLS), WCOLS)
            x = x_tile[slot, rows]
            gate = jnp.dot(x, gate_w[s, :, cols], preferred_element_type=jnp.float32)
            up = jnp.dot(x, up_w[s, :, cols], preferred_element_type=jnp.float32)
            hidden[s, rows, cols] = (jax.nn.silu(gate) * up).astype(jnp.bfloat16)
            return 0
        if piece == 0:
            for j in range(depth // WCOLS):
                chunk(j, 0)
        else:
            lax.fori_loop(0, depth // WCOLS, chunk, 0)

    def part(s, cols, rows=pl.ds(0, 2 * ROWS)):
        return jnp.dot(hidden[s, rows], down_w[s, :, cols], preferred_element_type=jnp.float32).astype(jnp.bfloat16)

    def both(slot, store):
        make_hidden(slot, 0)
        make_hidden(slot, 1)

        def chunk(j, _):
            cols = pl.ds(pl.multiple_of(j * YCOLS, YCOLS), YCOLS)
            store(cols, part(0, cols).astype(jnp.float32) + part(1, cols).astype(jnp.float32))
            return 0
        lax.fori_loop(0, width // YCOLS, chunk, 0)

    def start_pieces():
        for piece in pieces:
            piece_copy(*piece).start()

    for i in range(ROWS // FIRST):
        rows = pl.ds(i * 2 * FIRST, 2 * FIRST)
        for cp in piece_copies(i):
            cp.wait()
        make_hidden(0, core, piece=i)

        @pl.when(core == 1)
        def _(i=i, rows=rows):
            if i == 0:
                pl.semaphore_wait(barrier, 3)
            for j in range(width // YCOLS):
                if i == 0:
                    wait_load(depth // WCOLS + j)
                cols = pl.ds(j * YCOLS, YCOLS)
                y = part(1, cols, rows)
                for d in (RIGHT, LEFT):
                    result[1, d, pl.ds(i * FIRST, FIRST), cols] = y[d * FIRST:(d + 1) * FIRST]
                for d in (RIGHT, LEFT):
                    piece_copy(d, i, j).start()

        @pl.when(core == 0)
        def _(i=i):
            for j in range(width // YCOLS) if i == 0 else ():
                wait_load(depth // WCOLS + j)
            for d in (RIGHT, LEFT):
                result[0, d, pl.ds(i * FIRST, FIRST), pl.ds(0, depth)] = hidden[0, pl.ds((2 * i + d) * FIRST, FIRST)]
        if i == 0:
            own_gain.start()
            for cp in peer_w:
                cp.start()
            start_x(0, 1, 1)

    @pl.when(core == 0)
    def _():
        for d in (RIGHT, LEFT):
            mid_g(d, 0).start()

    def mid_step(stg, t, s):
        slot = lax.rem(t, 2)

        @pl.when(t < last)
        def _():
            start_x(stg, t + 1, 1 - slot)

        @pl.when(t == last)
        def _():
            start_x(stg + 1, 0, 1 - slot)
        wait_x(stg, t, slot)
        make_hidden(slot, s)

        @pl.when(s == 0)
        def _():
            for d in (RIGHT, LEFT):
                result[0, d, rows_of(t), pl.ds(0, depth)] = hidden[0, pl.ds(d * ROWS, ROWS)]
            for d in (RIGHT, LEFT):
                mid_g(d, t).start()

        @pl.when(s == 1)
        def _():
            def chunk(j, _):
                cols = pl.ds(pl.multiple_of(j * YCOLS, YCOLS), YCOLS)
                y = part(1, cols)
                for d in (RIGHT, LEFT):
                    result[1, d, rows_of(t), cols] = y[d * ROWS:(d + 1) * ROWS]
                return 0
            lax.fori_loop(0, width // YCOLS, chunk, 0)

            @pl.when(t == 0)
            def _():
                start_pieces()

            @pl.when(t > 0)
            def _():
                for d in (RIGHT, LEFT):
                    mid_y(d, t).start()

    def loop(t0, t1, step):
        def body(t, _):
            step(t)
            return 0
        lax.fori_loop(t0, t1, body, 0)

    loop(1, tiles, lambda t: mid_step(0, t, core))
    for cp in peer_w:
        cp.wait_recv()

    @pl.when(core == 1)
    def _():
        for d in (RIGHT, LEFT):
            down_copy(d, down_w.at[0, pl.ds(half_depth, half_depth)]).start()
    loop(0, tiles, lambda t: mid_step(1, t, 1 - core))

    def near_step(t):
        slot, place = lax.rem(t, 2), lax.rem(t, NEAR_SLOTS)

        for now, stg, nxt in ((0, 2, 1), (NEAR_SLOTS - 1, 4, 0), (NEAR_SLOTS, 2, NEAR_SLOTS + 1), (last, 3, 0)):
            @pl.when(t == now)
            def _(stg=stg, nxt=nxt):
                start_x(stg, nxt, 1 - slot)
        wait_x(2, t, slot)
        make_hidden(slot, 0)
        make_hidden(slot, 1)

        @pl.when(t >= NEAR_SLOTS)
        def _():
            for d in (RIGHT, LEFT):
                for cp in near_copies(d, t - NEAR_SLOTS, place):
                    cp.wait_send()
        for d in (RIGHT, LEFT):
            near_g[place, d] = hidden[0, pl.ds(d * ROWS, ROWS)]

        def chunk(j, _):
            cols = pl.ds(pl.multiple_of(j * YCOLS, YCOLS), YCOLS)
            y = part(1, cols)
            for d in (RIGHT, LEFT):
                near_y[place, d, :, cols] = y[d * ROWS:(d + 1) * ROWS]
            return 0
        lax.fori_loop(0, width // YCOLS, chunk, 0)
        for d in (RIGHT, LEFT):
            for cp in near_copies(d, t, place):
                cp.start()
    loop(0, NEAR_SLOTS, near_step)

    def own_step(t):
        slot = lax.rem(t, 2)

        @pl.when(t < last)
        def _():
            start_x(4, t + 1, 1 - slot)

        @pl.when(t == last)
        def _():
            start_x(2, NEAR_SLOTS, 1 - slot)
        wait_x(4, t, slot)
        res_copies = [pltpu.make_async_copy(
            residual.at[pl.ds(pl.multiple_of(h * half + t * ROWS, ROWS), ROWS)], y_tile.at[h], res_sem.at[h]) for h in (0, 1)]
        for cp in res_copies:
            cp.start()
        for cp in res_copies:
            cp.wait()

        def store(cols, y):
            for h in (0, 1):
                acc[h, rows_of(t), cols] = y[h * ROWS:(h + 1) * ROWS] + y_tile[h, :, cols].astype(jnp.float32)
        both(slot, store)

    loop(0, tiles, own_step)

    for d in (RIGHT, LEFT):
        down_copy(d, w_down.at[pl.ds(0, half_depth)]).wait_recv()
        swap_copy(d).start()
    for piece in pieces:
        piece_copy(*piece).wait_send()
    loop(0, tiles, lambda t: [mid_g(d, t).wait_send() for d in (RIGHT, LEFT)])
    loop(1, tiles, lambda t: [mid_y(d, t).wait_send() for d in (RIGHT, LEFT)])
    for d in (RIGHT, LEFT):
        swap_copy(d).wait_recv()
    loads = [pltpu.make_async_copy(down_in.at[d, pl.ds(h * half_depth, half_depth)], result.at[d, h], load_sem.at[d, h])
             for d in (RIGHT, LEFT) for h in (0, 1)]
    for cp in loads:
        cp.start()
    for cp in loads:
        cp.wait()

    loop(NEAR_SLOTS, tiles, near_step)


    def load_terms(kind, t):
        cps = []
        for d in (RIGHT, LEFT):
            cps.append(pltpu.make_async_copy(y_in.at[kind, d, rows_of(t)], y_tile.at[d], tile_sem.at[1, d]))
            cps.append(pltpu.make_async_copy(g_in.at[kind, d, rows_of(t)], g_tile.at[d], tile_sem.at[0, d]))
        return cps

    def term(d, cols):
        w = result[d, :, :, cols].reshape(depth, YCOLS)
        y = jnp.dot(g_tile[d], w, preferred_element_type=jnp.float32).astype(jnp.bfloat16)
        return y.astype(jnp.float32) + y_tile[d, :, cols].astype(jnp.float32)

    def far_tile(t, slot, place):
        wait_x(3, t, slot)

        def store(cols, y):
            for d in (RIGHT, LEFT):
                stage[place, d, :, cols] = y[d * ROWS:(d + 1) * ROWS]
        both(slot, store)
        for d in (RIGHT, LEFT):
            mid_g(d, t).wait_recv()

        @pl.when(t == 0)
        def _():
            for piece in pieces:
                piece_copy(*piece).wait_recv()

        @pl.when(t > 0)
        def _():
            for d in (RIGHT, LEFT):
                mid_y(d, t).wait_recv()
        for cp in load_terms(0, t):
            cp.start()
        for cp in load_terms(0, t):
            cp.wait()

        def chunk(j, _):
            cols = pl.ds(pl.multiple_of(j * YCOLS, YCOLS), YCOLS)
            for d in (RIGHT, LEFT):
                stage[place, d, :, cols] += term(d, cols)
            return 0
        lax.fori_loop(0, width // YCOLS, chunk, 0)

    def far_step(t):
        slot, place = lax.rem(t, 2), lax.rem(t, FAR_SLOTS)

        @pl.when(t < last)
        def _():
            start_x(3, t + 1, 1 - slot)

        @pl.when(t >= FAR_SLOTS)
        def _():
            for d in (RIGHT, LEFT):
                far_copy(d, t - FAR_SLOTS, place).wait_send()
        far_tile(t, slot, place)

        @pl.when(t < last)
        def _():
            for d in (RIGHT, LEFT):
                far_copy(d, t, place).start()

        @pl.when(t == last)
        def _():
            for i in range(ROWS // SUB):
                for d in (RIGHT, LEFT):
                    last_copy(d, i).start()
    loop(0, tiles, far_step)

    def own_terms(t):
        for d in (RIGHT, LEFT):
            for cp in near_copies(d, t, 0):
                cp.wait_recv()
        for cp in load_terms(1, t):
            cp.start()
        for cp in load_terms(1, t):
            cp.wait()

        def chunk(j, _):
            cols = pl.ds(pl.multiple_of(j * YCOLS, YCOLS), YCOLS)
            for h in (0, 1):
                acc[h, rows_of(t), cols] += term(1 - h, cols)
            return 0
        lax.fori_loop(0, width // YCOLS, chunk, 0)

    loop(0, tiles, own_terms)

    for cp in peer_w:
        cp.wait_send()
    for d in (RIGHT, LEFT):
        down_copy(d, w_down.at[pl.ds(0, half_depth)]).wait_send()
        swap_copy(d).wait_send()
        for place in range(NEAR_SLOTS):
            for cp in near_copies(d, 0, place):
                cp.wait_send()
    own_gain.wait()

    def finish(row):
        for h in (0, 1):
            here = pl.ds(row, 16)
            value = acc[h, here] + far_in[h, here]
            mean_sq = jnp.mean(value * value, axis=-1, keepdims=True)
            result[0, h, here] = value.astype(jnp.bfloat16)
            result[1, h, here] = (value * lax.rsqrt(mean_sq + EPS) * gain[...]).astype(jnp.bfloat16)

    def last_step(t):
        for d in (RIGHT, LEFT):
            far_copy(d, t, 0).wait_recv()
        loop(0, ROWS // 16, lambda j: finish(pl.multiple_of(t * ROWS + j * 16, 16)))
    loop(0, last, last_step)

    for place in range(FAR_SLOTS):
        if place != last_place:
            for d in (RIGHT, LEFT):
                far_copy(d, 0, place).wait_send()

    for i in range(ROWS // SUB):
        for d in (RIGHT, LEFT):
            last_copy(d, i).wait_recv()
        for j in range(SUB // 16):
            finish(last * ROWS + i * SUB + j * 16)
    for i in range(ROWS // SUB):
        for d in (RIGHT, LEFT):
            last_copy(d, i).wait_send()


def write_kernel(result, h_out, normed, sem):
    half = result.shape[2]
    copies = [
        pltpu.make_async_copy(result.at[i, h], out.at[pl.ds(h * half, half)], sem.at[i, h])
        for i, out in enumerate((h_out, normed)) for h in (0, 1)]
    for cp in copies:
        cp.start()
    for cp in copies:
        cp.wait()


def solution(mesh):
    n = mesh.shape["tp"]

    def local_block(x_in, w_gate, w_up, w_down, residual, norm_gain):
        rows, width = residual.shape
        depth = w_gate.shape[1]
        half = rows // 2
        tiles = half // ROWS
        f32, bf16 = jnp.float32, jnp.bfloat16
        dma = pltpu.SemaphoreType.DMA
        any_space = pl.BlockSpec(memory_space=pl.ANY)
        result, _, _, _ = pl.pallas_call(
            functools.partial(ring_kernel, n),
            out_shape=(
                pltpu.VMEM((2, 2, half, width), bf16),
                jax.ShapeDtypeStruct((2, 2, half, width), bf16),
                jax.ShapeDtypeStruct((2, 2, half, depth), bf16),
                jax.ShapeDtypeStruct((2, depth, width), bf16),
            ),
            in_specs=[any_space] * 6,
            out_specs=(pl.BlockSpec(memory_space=pltpu.VMEM),) + (any_space,) * 3,
            scratch_shapes=[
                pltpu.VMEM((2,) + w_gate.shape, bf16),
                pltpu.VMEM((2,) + w_up.shape, bf16),
                pltpu.VMEM((2,) + w_down.shape, bf16),
                pltpu.VMEM((2, 2 * ROWS, width), bf16),
                pltpu.VMEM((2, 2 * ROWS, depth), bf16),
                pltpu.VMEM((NEAR_SLOTS, 2, ROWS, width), bf16),
                pltpu.VMEM((NEAR_SLOTS, 2, ROWS, depth), bf16),
                pltpu.VMEM((FAR_SLOTS, 2, ROWS, width), f32),
                pltpu.VMEM((2, half, width), f32),
                pltpu.VMEM((2, half, width), f32),
                pltpu.VMEM((2, ROWS, width), bf16),
                pltpu.VMEM((2, ROWS, depth), bf16),
                pltpu.VMEM((1, width), f32),
                dma((depth // WCOLS,)), dma((depth // WCOLS,)), dma((width // YCOLS,)), dma(()), dma((2, 2)),
                dma((ROWS // FIRST, 2)), dma((2, 2)), dma((2,)),
                dma((3,)), dma((3,)),
                dma((2, ROWS // FIRST, width // YCOLS)), dma((2, ROWS // FIRST, width // YCOLS)),
                dma((2, 2, tiles)), dma((2, 2, tiles)),
                dma((NEAR_SLOTS, 2, 2)), dma((2, 2, tiles)),
                dma((FAR_SLOTS, 2)), dma((2, tiles)),
                dma((2, ROWS // SUB)), dma((2, ROWS // SUB)),
                dma((2,)), dma((2,)), dma((2,)), dma((2,)), dma((2, 2)),
            ],
            compiler_params=pltpu.CompilerParams(
                collective_id=0, has_side_effects=True, vmem_limit_bytes=VMEM_LIMIT),
            name="ring",
        )(x_in, w_gate, w_up, w_down, residual, norm_gain.reshape(1, width))
        return pl.pallas_call(
            write_kernel,
            out_shape=(jax.ShapeDtypeStruct((rows, width), bf16),) * 2,
            in_specs=[pl.BlockSpec(memory_space=pltpu.VMEM)],
            out_specs=(any_space, any_space),
            scratch_shapes=[dma((2, 2))],
            compiler_params=pltpu.CompilerParams(vmem_limit_bytes=2**20),
            name="write",
        )(pltpu.with_memory_space_constraint(result, pltpu.VMEM))

    row_spec = P(("data", "tp"), None)
    return jax.shard_map(local_block, mesh=mesh, in_specs=(P("data", None), P(None, "tp"), P(None, "tp"), P("tp", None), row_spec, P(None)), out_specs=(row_spec, row_spec), check_vma=False)
```

```python
import functools

import jax
import jax.numpy as jnp
from jax import lax
from jax.experimental import pallas as pl
from jax.experimental.pallas import tpu as pltpu
from jax.sharding import PartitionSpec as P

EPS = 1e-5
CORES = 2
ROWS = 128
FAR_SLOTS, NEAR_SLOTS = 3, 2
SUB = 32
FIRST = 64
WCOLS = 256
YCOLS = 512
AHEAD = 4
RIGHT, LEFT = 0, 1
VMEM_LIMIT = 58_500_000


def ring_kernel(
    n, x_in, w_gate, w_up, w_down, residual, norm_gain, result, y_in, g_in, down_in,
    gate_w, up_w, down_w, x_tile, hidden, near_y, near_g, stage, far_in, acc, y_tile, g_tile, gain,
    gate_sem, up_sem, down_sem, gain_sem, x_sem, piece_sem, tile_sem, res_sem,
    peer_send, peer_recv, first_send, first_recv, mid_send, mid_recv, near_send, near_recv, far_send, far_recv,
    last_send, last_recv, whole_send, whole_recv, swap_send, swap_recv, load_sem, partner_in,
):
    me = lax.axis_index("tp")
    chips = n // CORES
    chip, core = me // CORES, CORES - 1 - lax.rem(me, CORES)
    own_rows = residual.shape[0]
    half = own_rows // 2
    tiles = half // ROWS
    depth, width = w_gate.shape[1], w_down.shape[1]
    half_depth = depth // 2

    def position(c, k):
        return lax.rem(c + chips, chips) * CORES + CORES - 1 - k

    def device(c, k):
        return {"tp": position(c, k)}

    right, left, peer = device(chip + 1, core), device(chip - 1, core), device(chip, 1 - core)
    next_dev = (right, left)
    last = tiles - 1
    last_place = last % FAR_SLOTS

    barrier = pltpu.get_barrier_semaphore()

    def greet(dev, sem=barrier):
        pl.semaphore_signal(sem, inc=1, device_id=dev, device_id_type=pl.DeviceIdType.MESH)

    for dev in (left, right):
        greet(dev)

    @pl.when(core == 0)
    def _():
        greet(peer)

    def remote(src, dst, send, recv, dev):
        return pltpu.make_async_remote_copy(
            src_ref=src, dst_ref=dst, send_sem=send, recv_sem=recv, device_id=dev, device_id_type=pl.DeviceIdType.MESH)

    peer_w = [
        remote(w, dst.at[core], peer_send.at[i], peer_recv.at[i], peer)
        for i, (w, dst) in enumerate(((w_gate, gate_w), (w_up, up_w), (w_down, down_w)))]
    my_half = pl.ds(pl.multiple_of(core * half_depth, half_depth), half_depth)

    def down_copy(d, src):
        return remote(src, down_in.at[d, my_half], whole_send.at[d], whole_recv.at[d], next_dev[d])

    def swap_copy(d):
        return remote(down_in.at[d, my_half], down_in.at[d, my_half], swap_send.at[d], swap_recv.at[d], peer)

    @pl.when(core == 0)
    def _():
        pl.semaphore_wait(barrier, 2)
        for d in (RIGHT, LEFT):
            down_copy(d, w_down.at[pl.ds(0, half_depth)]).start()

    def x_copies(stg, t, slot):
        (c0, h0), (c1, h1) = (
            ((chip + 2, 0), (chip + 2, 1)),
            ((chip + 2, 0), (chip + 2, 1)),
            ((chip + 1, 1), (chip - 1, 0)),
            ((chip + 1, 0), (chip - 1, 1)),
            ((chip, 0), (chip, 1)),
        )[stg]
        out = []
        for d, (c, h) in enumerate(((c0, h0), (c1, h1))):
            row = pl.multiple_of(position(c, core) * own_rows + h * half + t * ROWS, ROWS)
            out.append(pltpu.make_async_copy(
                x_in.at[pl.ds(row, ROWS)], x_tile.at[slot, pl.ds(d * ROWS, ROWS)], x_sem.at[slot, d]))
        return out

    def start_x(stg, t, slot):
        for cp in x_copies(stg, t, slot):
            cp.start()

    def wait_x(stg, t, slot):
        for cp in x_copies(stg, t, slot):
            cp.wait()

    def piece_copies(i):
        out = []
        for d in (RIGHT, LEFT):
            row = pl.multiple_of(position(chip + 2, core) * own_rows + d * half + i * FIRST, FIRST)
            out.append(pltpu.make_async_copy(
                x_in.at[pl.ds(row, FIRST)], x_tile.at[0, pl.ds((2 * i + d) * FIRST, FIRST)], piece_sem.at[i, d]))
        return out

    def own_cols(j):
        cols = pl.ds(pl.multiple_of(j * WCOLS, WCOLS), WCOLS)
        return [
            pltpu.make_async_copy(w_gate.at[:, cols], gate_w.at[core, :, cols], gate_sem.at[j]),
            pltpu.make_async_copy(w_up.at[:, cols], up_w.at[core, :, cols], up_sem.at[j]),
        ]

    def own_down(j):
        cols = pl.ds(pl.multiple_of(j * YCOLS, YCOLS), YCOLS)
        return pltpu.make_async_copy(w_down.at[:, cols], down_w.at[core, :, cols], down_sem.at[j])

    own_gain = pltpu.make_async_copy(norm_gain, gain, gain_sem)
    loads = [own_cols(j) for j in range(depth // WCOLS)] + [[own_down(j)] for j in range(width // YCOLS)]

    def start_load(i):
        for cp in loads[i] if i < len(loads) else ():
            cp.start()

    def wait_load(i):
        for cp in loads[i]:
            cp.wait()
        start_load(i + AHEAD)

    for cp in piece_copies(0):
        cp.start()
    for i in range(AHEAD):
        start_load(i)
    for k in range(1, ROWS // FIRST):
        for cp in piece_copies(k):
            cp.start()

    def rows_of(t):
        return pl.ds(pl.multiple_of(t * ROWS, ROWS), ROWS)

    def mid_y(d, t):
        return remote(result.at[1, d, rows_of(t)], y_in.at[0, d, rows_of(t)], mid_send.at[1, d, t], mid_recv.at[1, d, t], next_dev[d])

    def mid_g(d, t):
        return remote(result.at[0, d, rows_of(t), pl.ds(0, depth)], g_in.at[0, d, rows_of(t)],
                      mid_send.at[0, d, t], mid_recv.at[0, d, t], next_dev[d])

    def near_copies(d, t, place):
        return [
            remote(near_g.at[place, d], g_in.at[1, d, rows_of(t)], near_send.at[place, d, 0], near_recv.at[0, d, t], next_dev[d]),
            remote(near_y.at[place, d], y_in.at[1, d, rows_of(t)], near_send.at[place, d, 1], near_recv.at[1, d, t], next_dev[d]),
        ]

    def far_copy(d, t, place):
        return remote(stage.at[place, d], far_in.at[d, rows_of(t)], far_send.at[place, d], far_recv.at[d, t], next_dev[d])

    def last_copy(d, i):
        here = pl.ds(last * ROWS + i * SUB, SUB)
        return remote(stage.at[last_place, d, pl.ds(i * SUB, SUB)], far_in.at[d, here],
                      last_send.at[d, i], last_recv.at[d, i], next_dev[d])

    def piece_copy(d, i, j):
        here, cols = pl.ds(i * FIRST, FIRST), pl.ds(j * YCOLS, YCOLS)
        return remote(result.at[1, d, here, cols], y_in.at[0, d, here, cols],
                      first_send.at[d, i, j], first_recv.at[d, i, j], next_dev[d])

    pieces = [(d, i, j) for i in range(ROWS // FIRST) for j in range(width // YCOLS) for d in (RIGHT, LEFT)]

    def make_hidden(slot, s, piece=None):
        rows = pl.ds(0, 2 * ROWS) if piece is None else pl.ds(piece * 2 * FIRST, 2 * FIRST)

        def chunk(j, _):
            if piece == 0:
                wait_load(j)
            cols = pl.ds(pl.multiple_of(j * WCOLS, WCOLS), WCOLS)
            x = x_tile[slot, rows]
            gate = jnp.dot(x, gate_w[s, :, cols], preferred_element_type=jnp.float32)
            up = jnp.dot(x, up_w[s, :, cols], preferred_element_type=jnp.float32)
            hidden[s, rows, cols] = (jax.nn.silu(gate) * up).astype(jnp.bfloat16)
            return 0
        if piece == 0:
            for j in range(depth // WCOLS):
                chunk(j, 0)
        else:
            lax.fori_loop(0, depth // WCOLS, chunk, 0)

    def part(s, cols, rows=pl.ds(0, 2 * ROWS)):
        return jnp.dot(hidden[s, rows], down_w[s, :, cols], preferred_element_type=jnp.float32).astype(jnp.bfloat16)

    def both(slot, store):
        make_hidden(slot, 0)
        make_hidden(slot, 1)

        def chunk(j, _):
            cols = pl.ds(pl.multiple_of(j * YCOLS, YCOLS), YCOLS)
            store(cols, part(0, cols).astype(jnp.float32) + part(1, cols).astype(jnp.float32))
            return 0
        lax.fori_loop(0, width // YCOLS, chunk, 0)

    def start_pieces():
        for piece in pieces:
            piece_copy(*piece).start()

    for i in range(ROWS // FIRST):
        rows = pl.ds(i * 2 * FIRST, 2 * FIRST)
        for cp in piece_copies(i):
            cp.wait()
        make_hidden(0, core, piece=i)

        @pl.when(core == 1)
        def _(i=i, rows=rows):
            if i == 0:
                pl.semaphore_wait(barrier, 3)
                greet(peer, partner_in)
            for j in range(width // YCOLS):
                if i == 0:
                    wait_load(depth // WCOLS + j)
                cols = pl.ds(j * YCOLS, YCOLS)
                y = part(1, cols, rows)
                for d in (RIGHT, LEFT):
                    result[1, d, pl.ds(i * FIRST, FIRST), cols] = y[d * FIRST:(d + 1) * FIRST]
                for d in (RIGHT, LEFT):
                    piece_copy(d, i, j).start()

        @pl.when(core == 0)
        def _(i=i):
            for j in range(width // YCOLS) if i == 0 else ():
                wait_load(depth // WCOLS + j)
            for d in (RIGHT, LEFT):
                result[0, d, pl.ds(i * FIRST, FIRST), pl.ds(0, depth)] = hidden[0, pl.ds((2 * i + d) * FIRST, FIRST)]
        if i == 0:
            own_gain.start()

            @pl.when(core == 0)
            def _():
                pl.semaphore_wait(partner_in, 1)
            for cp in peer_w:
                cp.start()
            start_x(0, 1, 1)

    @pl.when(core == 0)
    def _():
        for d in (RIGHT, LEFT):
            mid_g(d, 0).start()

    def mid_step(stg, t, s):
        slot = lax.rem(t, 2)

        @pl.when(t < last)
        def _():
            start_x(stg, t + 1, 1 - slot)

        @pl.when(t == last)
        def _():
            start_x(stg + 1, 0, 1 - slot)
        wait_x(stg, t, slot)
        make_hidden(slot, s)

        @pl.when(s == 0)
        def _():
            for d in (RIGHT, LEFT):
                result[0, d, rows_of(t), pl.ds(0, depth)] = hidden[0, pl.ds(d * ROWS, ROWS)]
            for d in (RIGHT, LEFT):
                mid_g(d, t).start()

        @pl.when(s == 1)
        def _():
            def chunk(j, _):
                cols = pl.ds(pl.multiple_of(j * YCOLS, YCOLS), YCOLS)
                y = part(1, cols)
                for d in (RIGHT, LEFT):
                    result[1, d, rows_of(t), cols] = y[d * ROWS:(d + 1) * ROWS]
                return 0
            lax.fori_loop(0, width // YCOLS, chunk, 0)

            @pl.when(t == 0)
            def _():
                start_pieces()

            @pl.when(t > 0)
            def _():
                for d in (RIGHT, LEFT):
                    mid_y(d, t).start()

    def loop(t0, t1, step):
        def body(t, _):
            step(t)
            return 0
        lax.fori_loop(t0, t1, body, 0)

    loop(1, tiles, lambda t: mid_step(0, t, core))
    for cp in peer_w:
        cp.wait_recv()

    @pl.when(core == 1)
    def _():
        for d in (RIGHT, LEFT):
            down_copy(d, down_w.at[0, pl.ds(half_depth, half_depth)]).start()
    loop(0, tiles, lambda t: mid_step(1, t, 1 - core))

    def near_step(t):
        slot, place = lax.rem(t, 2), lax.rem(t, NEAR_SLOTS)

        for now, stg, nxt in ((0, 2, 1), (NEAR_SLOTS - 1, 4, 0), (NEAR_SLOTS, 2, NEAR_SLOTS + 1), (last, 3, 0)):
            @pl.when(t == now)
            def _(stg=stg, nxt=nxt):
                start_x(stg, nxt, 1 - slot)
        wait_x(2, t, slot)
        make_hidden(slot, 0)
        make_hidden(slot, 1)

        @pl.when(t >= NEAR_SLOTS)
        def _():
            for d in (RIGHT, LEFT):
                for cp in near_copies(d, t - NEAR_SLOTS, place):
                    cp.wait_send()
        for d in (RIGHT, LEFT):
            near_g[place, d] = hidden[0, pl.ds(d * ROWS, ROWS)]

        def chunk(j, _):
            cols = pl.ds(pl.multiple_of(j * YCOLS, YCOLS), YCOLS)
            y = part(1, cols)
            for d in (RIGHT, LEFT):
                near_y[place, d, :, cols] = y[d * ROWS:(d + 1) * ROWS]
            return 0
        lax.fori_loop(0, width // YCOLS, chunk, 0)
        for d in (RIGHT, LEFT):
            for cp in near_copies(d, t, place):
                cp.start()
    loop(0, NEAR_SLOTS, near_step)

    def own_step(t):
        slot = lax.rem(t, 2)

        @pl.when(t < last)
        def _():
            start_x(4, t + 1, 1 - slot)

        @pl.when(t == last)
        def _():
            start_x(2, NEAR_SLOTS, 1 - slot)
        wait_x(4, t, slot)
        res_copies = [pltpu.make_async_copy(
            residual.at[pl.ds(pl.multiple_of(h * half + t * ROWS, ROWS), ROWS)], y_tile.at[h], res_sem.at[h]) for h in (0, 1)]
        for cp in res_copies:
            cp.start()
        for cp in res_copies:
            cp.wait()

        def store(cols, y):
            for h in (0, 1):
                acc[h, rows_of(t), cols] = y[h * ROWS:(h + 1) * ROWS] + y_tile[h, :, cols].astype(jnp.float32)
        both(slot, store)

    loop(0, tiles, own_step)

    for d in (RIGHT, LEFT):
        down_copy(d, w_down.at[pl.ds(0, half_depth)]).wait_recv()
        swap_copy(d).start()
    for piece in pieces:
        piece_copy(*piece).wait_send()
    loop(0, tiles, lambda t: [mid_g(d, t).wait_send() for d in (RIGHT, LEFT)])
    loop(1, tiles, lambda t: [mid_y(d, t).wait_send() for d in (RIGHT, LEFT)])
    for d in (RIGHT, LEFT):
        swap_copy(d).wait_recv()
    loads = [pltpu.make_async_copy(down_in.at[d, pl.ds(h * half_depth, half_depth)], result.at[d, h], load_sem.at[d, h])
             for d in (RIGHT, LEFT) for h in (0, 1)]
    for cp in loads:
        cp.start()
    for cp in loads:
        cp.wait()

    loop(NEAR_SLOTS, tiles, near_step)


    def load_terms(kind, t):
        cps = []
        for d in (RIGHT, LEFT):
            cps.append(pltpu.make_async_copy(y_in.at[kind, d, rows_of(t)], y_tile.at[d], tile_sem.at[1, d]))
            cps.append(pltpu.make_async_copy(g_in.at[kind, d, rows_of(t)], g_tile.at[d], tile_sem.at[0, d]))
        return cps

    def term(d, cols):
        w = result[d, :, :, cols].reshape(depth, YCOLS)
        y = jnp.dot(g_tile[d], w, preferred_element_type=jnp.float32).astype(jnp.bfloat16)
        return y.astype(jnp.float32) + y_tile[d, :, cols].astype(jnp.float32)

    def far_tile(t, slot, place):
        wait_x(3, t, slot)

        def store(cols, y):
            for d in (RIGHT, LEFT):
                stage[place, d, :, cols] = y[d * ROWS:(d + 1) * ROWS]
        both(slot, store)
        for d in (RIGHT, LEFT):
            mid_g(d, t).wait_recv()

        @pl.when(t == 0)
        def _():
            for piece in pieces:
                piece_copy(*piece).wait_recv()

        @pl.when(t > 0)
        def _():
            for d in (RIGHT, LEFT):
                mid_y(d, t).wait_recv()
        for cp in load_terms(0, t):
            cp.start()
        for cp in load_terms(0, t):
            cp.wait()

        def chunk(j, _):
            cols = pl.ds(pl.multiple_of(j * YCOLS, YCOLS), YCOLS)
            for d in (RIGHT, LEFT):
                stage[place, d, :, cols] += term(d, cols)
            return 0
        lax.fori_loop(0, width // YCOLS, chunk, 0)

    def far_step(t):
        slot, place = lax.rem(t, 2), lax.rem(t, FAR_SLOTS)

        @pl.when(t < last)
        def _():
            start_x(3, t + 1, 1 - slot)

        @pl.when(t >= FAR_SLOTS)
        def _():
            for d in (RIGHT, LEFT):
                far_copy(d, t - FAR_SLOTS, place).wait_send()
        far_tile(t, slot, place)

        @pl.when(t < last)
        def _():
            for d in (RIGHT, LEFT):
                far_copy(d, t, place).start()

        @pl.when(t == last)
        def _():
            for i in range(ROWS // SUB):
                for d in (RIGHT, LEFT):
                    last_copy(d, i).start()
    loop(0, tiles, far_step)

    def own_terms(t):
        for d in (RIGHT, LEFT):
            for cp in near_copies(d, t, 0):
                cp.wait_recv()
        for cp in load_terms(1, t):
            cp.start()
        for cp in load_terms(1, t):
            cp.wait()

        def chunk(j, _):
            cols = pl.ds(pl.multiple_of(j * YCOLS, YCOLS), YCOLS)
            for h in (0, 1):
                acc[h, rows_of(t), cols] += term(1 - h, cols)
            return 0
        lax.fori_loop(0, width // YCOLS, chunk, 0)

    loop(0, tiles, own_terms)

    for cp in peer_w:
        cp.wait_send()
    for d in (RIGHT, LEFT):
        down_copy(d, w_down.at[pl.ds(0, half_depth)]).wait_send()
        swap_copy(d).wait_send()
        for place in range(NEAR_SLOTS):
            for cp in near_copies(d, 0, place):
                cp.wait_send()
    own_gain.wait()

    def finish(row):
        for h in (0, 1):
            here = pl.ds(row, 16)
            value = acc[h, here] + far_in[h, here]
            mean_sq = jnp.mean(value * value, axis=-1, keepdims=True)
            result[0, h, here] = value.astype(jnp.bfloat16)
            result[1, h, here] = (value * lax.rsqrt(mean_sq + EPS) * gain[...]).astype(jnp.bfloat16)

    def last_step(t):
        for d in (RIGHT, LEFT):
            far_copy(d, t, 0).wait_recv()
        loop(0, ROWS // 16, lambda j: finish(pl.multiple_of(t * ROWS + j * 16, 16)))
    loop(0, last, last_step)

    for place in range(FAR_SLOTS):
        if place != last_place:
            for d in (RIGHT, LEFT):
                far_copy(d, 0, place).wait_send()

    for i in range(ROWS // SUB):
        for d in (RIGHT, LEFT):
            last_copy(d, i).wait_recv()
        for j in range(SUB // 16):
            finish(last * ROWS + i * SUB + j * 16)
    for i in range(ROWS // SUB):
        for d in (RIGHT, LEFT):
            last_copy(d, i).wait_send()


def write_kernel(result, h_out, normed, sem):
    half = result.shape[2]
    copies = [
        pltpu.make_async_copy(result.at[i, h], out.at[pl.ds(h * half, half)], sem.at[i, h])
        for i, out in enumerate((h_out, normed)) for h in (0, 1)]
    for cp in copies:
        cp.start()
    for cp in copies:
        cp.wait()


def solution(mesh):
    n = mesh.shape["tp"]

    def local_block(x_in, w_gate, w_up, w_down, residual, norm_gain):
        rows, width = residual.shape
        depth = w_gate.shape[1]
        half = rows // 2
        tiles = half // ROWS
        f32, bf16 = jnp.float32, jnp.bfloat16
        dma = pltpu.SemaphoreType.DMA
        any_space = pl.BlockSpec(memory_space=pl.ANY)
        result, _, _, _ = pl.pallas_call(
            functools.partial(ring_kernel, n),
            out_shape=(
                pltpu.VMEM((2, 2, half, width), bf16),
                jax.ShapeDtypeStruct((2, 2, half, width), bf16),
                jax.ShapeDtypeStruct((2, 2, half, depth), bf16),
                jax.ShapeDtypeStruct((2, depth, width), bf16),
            ),
            in_specs=[any_space] * 6,
            out_specs=(pl.BlockSpec(memory_space=pltpu.VMEM),) + (any_space,) * 3,
            scratch_shapes=[
                pltpu.VMEM((2,) + w_gate.shape, bf16),
                pltpu.VMEM((2,) + w_up.shape, bf16),
                pltpu.VMEM((2,) + w_down.shape, bf16),
                pltpu.VMEM((2, 2 * ROWS, width), bf16),
                pltpu.VMEM((2, 2 * ROWS, depth), bf16),
                pltpu.VMEM((NEAR_SLOTS, 2, ROWS, width), bf16),
                pltpu.VMEM((NEAR_SLOTS, 2, ROWS, depth), bf16),
                pltpu.VMEM((FAR_SLOTS, 2, ROWS, width), f32),
                pltpu.VMEM((2, half, width), f32),
                pltpu.VMEM((2, half, width), f32),
                pltpu.VMEM((2, ROWS, width), bf16),
                pltpu.VMEM((2, ROWS, depth), bf16),
                pltpu.VMEM((1, width), f32),
                dma((depth // WCOLS,)), dma((depth // WCOLS,)), dma((width // YCOLS,)), dma(()), dma((2, 2)),
                dma((ROWS // FIRST, 2)), dma((2, 2)), dma((2,)),
                dma((3,)), dma((3,)),
                dma((2, ROWS // FIRST, width // YCOLS)), dma((2, ROWS // FIRST, width // YCOLS)),
                dma((2, 2, tiles)), dma((2, 2, tiles)),
                dma((NEAR_SLOTS, 2, 2)), dma((2, 2, tiles)),
                dma((FAR_SLOTS, 2)), dma((2, tiles)),
                dma((2, ROWS // SUB)), dma((2, ROWS // SUB)),
                dma((2,)), dma((2,)), dma((2,)), dma((2,)), dma((2, 2)), pltpu.SemaphoreType.REGULAR,
            ],
            compiler_params=pltpu.CompilerParams(
                collective_id=0, has_side_effects=True, vmem_limit_bytes=VMEM_LIMIT),
            name="ring",
        )(x_in, w_gate, w_up, w_down, residual, norm_gain.reshape(1, width))
        return pl.pallas_call(
            write_kernel,
            out_shape=(jax.ShapeDtypeStruct((rows, width), bf16),) * 2,
            in_specs=[pl.BlockSpec(memory_space=pltpu.VMEM)],
            out_specs=(any_space, any_space),
            scratch_shapes=[dma((2, 2))],
            compiler_params=pltpu.CompilerParams(vmem_limit_bytes=2**20),
            name="write",
        )(pltpu.with_memory_space_constraint(result, pltpu.VMEM))

    row_spec = P(("data", "tp"), None)
    return jax.shard_map(local_block, mesh=mesh, in_specs=(P("data", None), P(None, "tp"), P(None, "tp"), P("tp", None), row_spec, P(None)), out_specs=(row_spec, row_spec), check_vma=False)
```

```python
import functools

import jax
import jax.numpy as jnp
from jax import lax
from jax.experimental import pallas as pl
from jax.experimental.pallas import tpu as pltpu
from jax.sharding import PartitionSpec as P

EPS = 1e-5
CORES = 2
ROWS = 128
FAR_SLOTS, NEAR_SLOTS = 3, 2
SUB = 32
FIRST = 64
WCOLS = 256
YCOLS = 512
AHEAD = 8
RIGHT, LEFT = 0, 1
VMEM_LIMIT = 58_500_000


def ring_kernel(
    n, x_in, w_gate, w_up, w_down, residual, norm_gain, result, y_in, g_in, down_in,
    gate_w, up_w, down_w, x_tile, hidden, near_y, near_g, stage, far_in, acc, y_tile, g_tile, gain,
    gate_sem, up_sem, down_sem, gain_sem, x_sem, piece_sem, tile_sem, res_sem,
    peer_send, peer_recv, first_send, first_recv, mid_send, mid_recv, near_send, near_recv, far_send, far_recv,
    last_send, last_recv, whole_send, whole_recv, swap_send, swap_recv, load_sem, partner_in,
):
    me = lax.axis_index("tp")
    chips = n // CORES
    chip, core = me // CORES, CORES - 1 - lax.rem(me, CORES)
    own_rows = residual.shape[0]
    half = own_rows // 2
    tiles = half // ROWS
    depth, width = w_gate.shape[1], w_down.shape[1]
    half_depth = depth // 2

    def position(c, k):
        return lax.rem(c + chips, chips) * CORES + CORES - 1 - k

    def device(c, k):
        return {"tp": position(c, k)}

    right, left, peer = device(chip + 1, core), device(chip - 1, core), device(chip, 1 - core)
    next_dev = (right, left)
    last = tiles - 1
    last_place = last % FAR_SLOTS

    barrier = pltpu.get_barrier_semaphore()

    def greet(dev, sem=barrier):
        pl.semaphore_signal(sem, inc=1, device_id=dev, device_id_type=pl.DeviceIdType.MESH)

    for dev in (left, right):
        greet(dev)

    @pl.when(core == 0)
    def _():
        greet(peer)

    def remote(src, dst, send, recv, dev):
        return pltpu.make_async_remote_copy(
            src_ref=src, dst_ref=dst, send_sem=send, recv_sem=recv, device_id=dev, device_id_type=pl.DeviceIdType.MESH)

    peer_w = [
        remote(w, dst.at[core], peer_send.at[i], peer_recv.at[i], peer)
        for i, (w, dst) in enumerate(((w_gate, gate_w), (w_up, up_w), (w_down, down_w)))]
    my_half = pl.ds(pl.multiple_of(core * half_depth, half_depth), half_depth)

    def down_copy(d, src):
        return remote(src, down_in.at[d, my_half], whole_send.at[d], whole_recv.at[d], next_dev[d])

    def swap_copy(d):
        return remote(down_in.at[d, my_half], down_in.at[d, my_half], swap_send.at[d], swap_recv.at[d], peer)

    @pl.when(core == 0)
    def _():
        pl.semaphore_wait(barrier, 2)
        for d in (RIGHT, LEFT):
            down_copy(d, w_down.at[pl.ds(0, half_depth)]).start()

    def x_copies(stg, t, slot):
        (c0, h0), (c1, h1) = (
            ((chip + 2, 0), (chip + 2, 1)),
            ((chip + 2, 0), (chip + 2, 1)),
            ((chip + 1, 1), (chip - 1, 0)),
            ((chip + 1, 0), (chip - 1, 1)),
            ((chip, 0), (chip, 1)),
        )[stg]
        out = []
        for d, (c, h) in enumerate(((c0, h0), (c1, h1))):
            row = pl.multiple_of(position(c, core) * own_rows + h * half + t * ROWS, ROWS)
            out.append(pltpu.make_async_copy(
                x_in.at[pl.ds(row, ROWS)], x_tile.at[slot, pl.ds(d * ROWS, ROWS)], x_sem.at[slot, d]))
        return out

    def start_x(stg, t, slot):
        for cp in x_copies(stg, t, slot):
            cp.start()

    def wait_x(stg, t, slot):
        for cp in x_copies(stg, t, slot):
            cp.wait()

    def piece_copies(i):
        out = []
        for d in (RIGHT, LEFT):
            row = pl.multiple_of(position(chip + 2, core) * own_rows + d * half + i * FIRST, FIRST)
            out.append(pltpu.make_async_copy(
                x_in.at[pl.ds(row, FIRST)], x_tile.at[0, pl.ds((2 * i + d) * FIRST, FIRST)], piece_sem.at[i, d]))
        return out

    def own_cols(j):
        cols = pl.ds(pl.multiple_of(j * WCOLS, WCOLS), WCOLS)
        return [
            pltpu.make_async_copy(w_gate.at[:, cols], gate_w.at[core, :, cols], gate_sem.at[j]),
            pltpu.make_async_copy(w_up.at[:, cols], up_w.at[core, :, cols], up_sem.at[j]),
        ]

    def own_down(j):
        cols = pl.ds(pl.multiple_of(j * YCOLS, YCOLS), YCOLS)
        return pltpu.make_async_copy(w_down.at[:, cols], down_w.at[core, :, cols], down_sem.at[j])

    own_gain = pltpu.make_async_copy(norm_gain, gain, gain_sem)
    loads = [own_cols(j) for j in range(depth // WCOLS)] + [[own_down(j)] for j in range(width // YCOLS)]

    def start_load(i):
        for cp in loads[i] if i < len(loads) else ():
            cp.start()

    def wait_load(i):
        for cp in loads[i]:
            cp.wait()
        start_load(i + AHEAD)

    for cp in piece_copies(0):
        cp.start()
    for i in range(AHEAD):
        start_load(i)
    for k in range(1, ROWS // FIRST):
        for cp in piece_copies(k):
            cp.start()

    def rows_of(t):
        return pl.ds(pl.multiple_of(t * ROWS, ROWS), ROWS)

    def mid_y(d, t):
        return remote(result.at[1, d, rows_of(t)], y_in.at[0, d, rows_of(t)], mid_send.at[1, d, t], mid_recv.at[1, d, t], next_dev[d])

    def mid_g(d, t):
        return remote(result.at[0, d, rows_of(t), pl.ds(0, depth)], g_in.at[0, d, rows_of(t)],
                      mid_send.at[0, d, t], mid_recv.at[0, d, t], next_dev[d])

    def near_copies(d, t, place):
        return [
            remote(near_g.at[place, d], g_in.at[1, d, rows_of(t)], near_send.at[place, d, 0], near_recv.at[0, d, t], next_dev[d]),
            remote(near_y.at[place, d], y_in.at[1, d, rows_of(t)], near_send.at[place, d, 1], near_recv.at[1, d, t], next_dev[d]),
        ]

    def far_copy(d, t, place):
        return remote(stage.at[place, d], far_in.at[d, rows_of(t)], far_send.at[place, d], far_recv.at[d, t], next_dev[d])

    def last_copy(d, i):
        here = pl.ds(last * ROWS + i * SUB, SUB)
        return remote(stage.at[last_place, d, pl.ds(i * SUB, SUB)], far_in.at[d, here],
                      last_send.at[d, i], last_recv.at[d, i], next_dev[d])

    def piece_copy(d, i, j):
        here, cols = pl.ds(i * FIRST, FIRST), pl.ds(j * YCOLS, YCOLS)
        return remote(result.at[1, d, here, cols], y_in.at[0, d, here, cols],
                      first_send.at[d, i, j], first_recv.at[d, i, j], next_dev[d])

    pieces = [(d, i, j) for i in range(ROWS // FIRST) for j in range(width // YCOLS) for d in (RIGHT, LEFT)]

    def make_hidden(slot, s, piece=None):
        rows = pl.ds(0, 2 * ROWS) if piece is None else pl.ds(piece * 2 * FIRST, 2 * FIRST)

        def chunk(j, _):
            if piece == 0:
                wait_load(j)
            cols = pl.ds(pl.multiple_of(j * WCOLS, WCOLS), WCOLS)
            x = x_tile[slot, rows]
            gate = jnp.dot(x, gate_w[s, :, cols], preferred_element_type=jnp.float32)
            up = jnp.dot(x, up_w[s, :, cols], preferred_element_type=jnp.float32)
            hidden[s, rows, cols] = (jax.nn.silu(gate) * up).astype(jnp.bfloat16)
            return 0
        if piece == 0:
            for j in range(depth // WCOLS):
                chunk(j, 0)
        else:
            lax.fori_loop(0, depth // WCOLS, chunk, 0)

    def part(s, cols, rows=pl.ds(0, 2 * ROWS)):
        return jnp.dot(hidden[s, rows], down_w[s, :, cols], preferred_element_type=jnp.float32).astype(jnp.bfloat16)

    def both(slot, store):
        make_hidden(slot, 0)
        make_hidden(slot, 1)

        def chunk(j, _):
            cols = pl.ds(pl.multiple_of(j * YCOLS, YCOLS), YCOLS)
            store(cols, part(0, cols).astype(jnp.float32) + part(1, cols).astype(jnp.float32))
            return 0
        lax.fori_loop(0, width // YCOLS, chunk, 0)

    def start_pieces():
        for piece in pieces:
            piece_copy(*piece).start()

    for i in range(ROWS // FIRST):
        rows = pl.ds(i * 2 * FIRST, 2 * FIRST)
        for cp in piece_copies(i):
            cp.wait()
        make_hidden(0, core, piece=i)

        @pl.when(core == 1)
        def _(i=i, rows=rows):
            if i == 0:
                pl.semaphore_wait(barrier, 3)
                greet(peer, partner_in)
            for j in range(width // YCOLS):
                if i == 0:
                    wait_load(depth // WCOLS + j)
                cols = pl.ds(j * YCOLS, YCOLS)
                y = part(1, cols, rows)
                for d in (RIGHT, LEFT):
                    result[1, d, pl.ds(i * FIRST, FIRST), cols] = y[d * FIRST:(d + 1) * FIRST]
                for d in (RIGHT, LEFT):
                    piece_copy(d, i, j).start()

        @pl.when(core == 0)
        def _(i=i):
            for j in range(width // YCOLS) if i == 0 else ():
                wait_load(depth // WCOLS + j)
            for d in (RIGHT, LEFT):
                result[0, d, pl.ds(i * FIRST, FIRST), pl.ds(0, depth)] = hidden[0, pl.ds((2 * i + d) * FIRST, FIRST)]
        if i == 0:
            own_gain.start()

            @pl.when(core == 0)
            def _():
                pl.semaphore_wait(partner_in, 1)
            for cp in peer_w:
                cp.start()
            start_x(0, 1, 1)

    @pl.when(core == 0)
    def _():
        for d in (RIGHT, LEFT):
            mid_g(d, 0).start()

    def mid_step(stg, t, s):
        slot = lax.rem(t, 2)

        @pl.when(t < last)
        def _():
            start_x(stg, t + 1, 1 - slot)

        @pl.when(t == last)
        def _():
            start_x(stg + 1, 0, 1 - slot)
        wait_x(stg, t, slot)
        make_hidden(slot, s)

        @pl.when(s == 0)
        def _():
            for d in (RIGHT, LEFT):
                result[0, d, rows_of(t), pl.ds(0, depth)] = hidden[0, pl.ds(d * ROWS, ROWS)]
            for d in (RIGHT, LEFT):
                mid_g(d, t).start()

        @pl.when(s == 1)
        def _():
            def chunk(j, _):
                cols = pl.ds(pl.multiple_of(j * YCOLS, YCOLS), YCOLS)
                y = part(1, cols)
                for d in (RIGHT, LEFT):
                    result[1, d, rows_of(t), cols] = y[d * ROWS:(d + 1) * ROWS]
                return 0
            lax.fori_loop(0, width // YCOLS, chunk, 0)

            @pl.when(t == 0)
            def _():
                start_pieces()

            @pl.when(t > 0)
            def _():
                for d in (RIGHT, LEFT):
                    mid_y(d, t).start()

    def loop(t0, t1, step):
        def body(t, _):
            step(t)
            return 0
        lax.fori_loop(t0, t1, body, 0)

    loop(1, tiles, lambda t: mid_step(0, t, core))
    for cp in peer_w:
        cp.wait_recv()

    @pl.when(core == 1)
    def _():
        for d in (RIGHT, LEFT):
            down_copy(d, down_w.at[0, pl.ds(half_depth, half_depth)]).start()
    loop(0, tiles, lambda t: mid_step(1, t, 1 - core))

    def near_step(t):
        slot, place = lax.rem(t, 2), lax.rem(t, NEAR_SLOTS)

        for now, stg, nxt in ((0, 2, 1), (NEAR_SLOTS - 1, 4, 0), (NEAR_SLOTS, 2, NEAR_SLOTS + 1), (last, 3, 0)):
            @pl.when(t == now)
            def _(stg=stg, nxt=nxt):
                start_x(stg, nxt, 1 - slot)
        wait_x(2, t, slot)
        make_hidden(slot, 0)
        make_hidden(slot, 1)

        @pl.when(t >= NEAR_SLOTS)
        def _():
            for d in (RIGHT, LEFT):
                for cp in near_copies(d, t - NEAR_SLOTS, place):
                    cp.wait_send()
        for d in (RIGHT, LEFT):
            near_g[place, d] = hidden[0, pl.ds(d * ROWS, ROWS)]

        def chunk(j, _):
            cols = pl.ds(pl.multiple_of(j * YCOLS, YCOLS), YCOLS)
            y = part(1, cols)
            for d in (RIGHT, LEFT):
                near_y[place, d, :, cols] = y[d * ROWS:(d + 1) * ROWS]
            return 0
        lax.fori_loop(0, width // YCOLS, chunk, 0)
        for d in (RIGHT, LEFT):
            for cp in near_copies(d, t, place):
                cp.start()
    loop(0, NEAR_SLOTS, near_step)

    def own_step(t):
        slot = lax.rem(t, 2)

        @pl.when(t < last)
        def _():
            start_x(4, t + 1, 1 - slot)

        @pl.when(t == last)
        def _():
            start_x(2, NEAR_SLOTS, 1 - slot)
        wait_x(4, t, slot)
        res_copies = [pltpu.make_async_copy(
            residual.at[pl.ds(pl.multiple_of(h * half + t * ROWS, ROWS), ROWS)], y_tile.at[h], res_sem.at[h]) for h in (0, 1)]
        for cp in res_copies:
            cp.start()
        for cp in res_copies:
            cp.wait()

        def store(cols, y):
            for h in (0, 1):
                acc[h, rows_of(t), cols] = y[h * ROWS:(h + 1) * ROWS] + y_tile[h, :, cols].astype(jnp.float32)
        both(slot, store)

    loop(0, tiles, own_step)

    for d in (RIGHT, LEFT):
        down_copy(d, w_down.at[pl.ds(0, half_depth)]).wait_recv()
        swap_copy(d).start()
    for piece in pieces:
        piece_copy(*piece).wait_send()
    loop(0, tiles, lambda t: [mid_g(d, t).wait_send() for d in (RIGHT, LEFT)])
    loop(1, tiles, lambda t: [mid_y(d, t).wait_send() for d in (RIGHT, LEFT)])
    for d in (RIGHT, LEFT):
        swap_copy(d).wait_recv()
    loads = [pltpu.make_async_copy(down_in.at[d, pl.ds(h * half_depth, half_depth)], result.at[d, h], load_sem.at[d, h])
             for d in (RIGHT, LEFT) for h in (0, 1)]
    for cp in loads:
        cp.start()
    for cp in loads:
        cp.wait()

    loop(NEAR_SLOTS, tiles, near_step)


    def load_terms(kind, t):
        cps = []
        for d in (RIGHT, LEFT):
            cps.append(pltpu.make_async_copy(y_in.at[kind, d, rows_of(t)], y_tile.at[d], tile_sem.at[1, d]))
            cps.append(pltpu.make_async_copy(g_in.at[kind, d, rows_of(t)], g_tile.at[d], tile_sem.at[0, d]))
        return cps

    def term(d, cols):
        w = result[d, :, :, cols].reshape(depth, YCOLS)
        y = jnp.dot(g_tile[d], w, preferred_element_type=jnp.float32).astype(jnp.bfloat16)
        return y.astype(jnp.float32) + y_tile[d, :, cols].astype(jnp.float32)

    def far_tile(t, slot, place):
        wait_x(3, t, slot)

        def store(cols, y):
            for d in (RIGHT, LEFT):
                stage[place, d, :, cols] = y[d * ROWS:(d + 1) * ROWS]
        both(slot, store)
        for d in (RIGHT, LEFT):
            mid_g(d, t).wait_recv()

        @pl.when(t == 0)
        def _():
            for piece in pieces:
                piece_copy(*piece).wait_recv()

        @pl.when(t > 0)
        def _():
            for d in (RIGHT, LEFT):
                mid_y(d, t).wait_recv()
        for cp in load_terms(0, t):
            cp.start()
        for cp in load_terms(0, t):
            cp.wait()

        def chunk(j, _):
            cols = pl.ds(pl.multiple_of(j * YCOLS, YCOLS), YCOLS)
            for d in (RIGHT, LEFT):
                stage[place, d, :, cols] += term(d, cols)
            return 0
        lax.fori_loop(0, width // YCOLS, chunk, 0)

    def far_step(t):
        slot, place = lax.rem(t, 2), lax.rem(t, FAR_SLOTS)

        @pl.when(t < last)
        def _():
            start_x(3, t + 1, 1 - slot)

        @pl.when(t >= FAR_SLOTS)
        def _():
            for d in (RIGHT, LEFT):
                far_copy(d, t - FAR_SLOTS, place).wait_send()
        far_tile(t, slot, place)

        @pl.when(t < last)
        def _():
            for d in (RIGHT, LEFT):
                far_copy(d, t, place).start()

        @pl.when(t == last)
        def _():
            for i in range(ROWS // SUB):
                for d in (RIGHT, LEFT):
                    last_copy(d, i).start()
    loop(0, tiles, far_step)

    def own_terms(t):
        for d in (RIGHT, LEFT):
            for cp in near_copies(d, t, 0):
                cp.wait_recv()
        for cp in load_terms(1, t):
            cp.start()
        for cp in load_terms(1, t):
            cp.wait()

        def chunk(j, _):
            cols = pl.ds(pl.multiple_of(j * YCOLS, YCOLS), YCOLS)
            for h in (0, 1):
                acc[h, rows_of(t), cols] += term(1 - h, cols)
            return 0
        lax.fori_loop(0, width // YCOLS, chunk, 0)

    loop(0, tiles, own_terms)

    for cp in peer_w:
        cp.wait_send()
    for d in (RIGHT, LEFT):
        down_copy(d, w_down.at[pl.ds(0, half_depth)]).wait_send()
        swap_copy(d).wait_send()
        for place in range(NEAR_SLOTS):
            for cp in near_copies(d, 0, place):
                cp.wait_send()
    own_gain.wait()

    def finish(row):
        for h in (0, 1):
            here = pl.ds(row, 16)
            value = acc[h, here] + far_in[h, here]
            mean_sq = jnp.mean(value * value, axis=-1, keepdims=True)
            result[0, h, here] = value.astype(jnp.bfloat16)
            result[1, h, here] = (value * lax.rsqrt(mean_sq + EPS) * gain[...]).astype(jnp.bfloat16)

    def last_step(t):
        for d in (RIGHT, LEFT):
            far_copy(d, t, 0).wait_recv()
        loop(0, ROWS // 16, lambda j: finish(pl.multiple_of(t * ROWS + j * 16, 16)))
    loop(0, last, last_step)

    for place in range(FAR_SLOTS):
        if place != last_place:
            for d in (RIGHT, LEFT):
                far_copy(d, 0, place).wait_send()

    for i in range(ROWS // SUB):
        for d in (RIGHT, LEFT):
            last_copy(d, i).wait_recv()
        for j in range(SUB // 16):
            finish(last * ROWS + i * SUB + j * 16)
    for i in range(ROWS // SUB):
        for d in (RIGHT, LEFT):
            last_copy(d, i).wait_send()


def write_kernel(result, h_out, normed, sem):
    half = result.shape[2]
    copies = [
        pltpu.make_async_copy(result.at[i, h], out.at[pl.ds(h * half, half)], sem.at[i, h])
        for i, out in enumerate((h_out, normed)) for h in (0, 1)]
    for cp in copies:
        cp.start()
    for cp in copies:
        cp.wait()


def solution(mesh):
    n = mesh.shape["tp"]

    def local_block(x_in, w_gate, w_up, w_down, residual, norm_gain):
        rows, width = residual.shape
        depth = w_gate.shape[1]
        half = rows // 2
        tiles = half // ROWS
        f32, bf16 = jnp.float32, jnp.bfloat16
        dma = pltpu.SemaphoreType.DMA
        any_space = pl.BlockSpec(memory_space=pl.ANY)
        result, _, _, _ = pl.pallas_call(
            functools.partial(ring_kernel, n),
            out_shape=(
                pltpu.VMEM((2, 2, half, width), bf16),
                jax.ShapeDtypeStruct((2, 2, half, width), bf16),
                jax.ShapeDtypeStruct((2, 2, half, depth), bf16),
                jax.ShapeDtypeStruct((2, depth, width), bf16),
            ),
            in_specs=[any_space] * 6,
            out_specs=(pl.BlockSpec(memory_space=pltpu.VMEM),) + (any_space,) * 3,
            scratch_shapes=[
                pltpu.VMEM((2,) + w_gate.shape, bf16),
                pltpu.VMEM((2,) + w_up.shape, bf16),
                pltpu.VMEM((2,) + w_down.shape, bf16),
                pltpu.VMEM((2, 2 * ROWS, width), bf16),
                pltpu.VMEM((2, 2 * ROWS, depth), bf16),
                pltpu.VMEM((NEAR_SLOTS, 2, ROWS, width), bf16),
                pltpu.VMEM((NEAR_SLOTS, 2, ROWS, depth), bf16),
                pltpu.VMEM((FAR_SLOTS, 2, ROWS, width), f32),
                pltpu.VMEM((2, half, width), f32),
                pltpu.VMEM((2, half, width), f32),
                pltpu.VMEM((2, ROWS, width), bf16),
                pltpu.VMEM((2, ROWS, depth), bf16),
                pltpu.VMEM((1, width), f32),
                dma((depth // WCOLS,)), dma((depth // WCOLS,)), dma((width // YCOLS,)), dma(()), dma((2, 2)),
                dma((ROWS // FIRST, 2)), dma((2, 2)), dma((2,)),
                dma((3,)), dma((3,)),
                dma((2, ROWS // FIRST, width // YCOLS)), dma((2, ROWS // FIRST, width // YCOLS)),
                dma((2, 2, tiles)), dma((2, 2, tiles)),
                dma((NEAR_SLOTS, 2, 2)), dma((2, 2, tiles)),
                dma((FAR_SLOTS, 2)), dma((2, tiles)),
                dma((2, ROWS // SUB)), dma((2, ROWS // SUB)),
                dma((2,)), dma((2,)), dma((2,)), dma((2,)), dma((2, 2)), pltpu.SemaphoreType.REGULAR,
            ],
            compiler_params=pltpu.CompilerParams(
                collective_id=0, has_side_effects=True, vmem_limit_bytes=VMEM_LIMIT),
            name="ring",
        )(x_in, w_gate, w_up, w_down, residual, norm_gain.reshape(1, width))
        return pl.pallas_call(
            write_kernel,
            out_shape=(jax.ShapeDtypeStruct((rows, width), bf16),) * 2,
            in_specs=[pl.BlockSpec(memory_space=pltpu.VMEM)],
            out_specs=(any_space, any_space),
            scratch_shapes=[dma((2, 2))],
            compiler_params=pltpu.CompilerParams(vmem_limit_bytes=2**20),
            name="write",
        )(pltpu.with_memory_space_constraint(result, pltpu.VMEM))

    row_spec = P(("data", "tp"), None)
    return jax.shard_map(local_block, mesh=mesh, in_specs=(P("data", None), P(None, "tp"), P(None, "tp"), P("tp", None), row_spec, P(None)), out_specs=(row_spec, row_spec), check_vma=False)
```
